32 devices in a mesh: lon: 4 (over y, x), lat: 4 (over z), mem: 2 (over core).
Axes of the slice: x: 2, y: 2, z: 4, core: 2. Of those that a mesh axis runs over, the one named last changes fastest.
Arguments:
- north_vel: bfloat16 [2, 4, 75, 128, 512], P('mem', None, None, 'lat', 'lon'), may hold values from -6 to 6
- up_vel: bfloat16 [2, 4, 75, 128, 512], P('mem', None, None, 'lat', 'lon'), may hold values from -6 to 6
- dens_class: int32 [2, 4, 75, 128, 512], P('mem', None, None, 'lat', 'lon'), may hold values from 0 to 79
- thickness: int32 [75, 128, 512], P(None, 'lat', 'lon'), may hold values from 0 to 2000
- basin_id: int32 [128, 512], P('lat', 'lon'), may hold values from 0 to 3
Outputs:
- depth_mean: float32 [4, 4, 2, 75, 128], P('lon', None, None, None, 'lat')
- depth_spread: float32 [4, 4, 2, 75, 128], P('lon', None, None, None, 'lat')
- class_mean: float32 [4, 4, 2, 80, 128], P('lon', None, None, None, 'lat')
- class_spread: float32 [4, 4, 2, 80, 128], P('lon', None, None, None, 'lat')
The draws below stay inside these ranges and needn't reach their ends.
Inputs may be any that keep to these rules, and one draw needn't show every extreme that they name: `basin_id`: 0 marks land; 1 to 3 name the basins. `thickness`: thousandths of a unit layer; 0 marks a cell below the sea floor.
All inputs are finite; a program needn't handle non-finite values.
Results may differ from the reference program's by a relative error of at most 0.0029.
Values sent between devices are 32-bit elements; how exact they have to be, the bound alone decides.
A program may use at most 128 MiB of HBM per device.

```python
import math
import jax
import jax.numpy as jnp
from jax import lax

MONTHS = 4
LEVELS = 75
CLASSES = 80
BASINS = 3
NLON = 512
NLAT = 128
MEMBERS = 2


def place_ends(array, rng, least, top_value):
    extent = array.shape
    index_at = [jax.random.randint(jax.random.fold_in(rng, axis), (), 0, extent[axis]) for axis in range(len(extent))]
    array = array.at[tuple(index_at)].set(least)
    longest = extent.index(max(extent))
    index_at[longest] = (index_at[longest] + 1) % extent[longest]
    return array.at[tuple(index_at)].set(top_value)


def level_of(own_key, extent, shards, low, top_value):
    factor_of, own = 1.0, jax.random.fold_in(own_key, 6)
    for position, shards_of in shards:
        heights = jnp.exp(jax.random.uniform(jax.random.fold_in(own, position), (shards_of,), jnp.float32, low / len(shards), top_value / len(shards)))
        factor_of = factor_of * jnp.repeat(heights, extent[position] // shards_of).reshape([-1 if axis == position else 1 for axis in range(len(extent))])
    return factor_of


def scatter_about(own_key, shape, width, most, pieces=(), held_as=jnp.bfloat16):
    entries = width * jax.random.normal(own_key, shape, jnp.float32)
    if pieces:
        entries = entries * level_of(own_key, shape, pieces, -0.22, 0.18)
    return jnp.clip(entries, -most, most).astype(held_as)


def setup_inputs(seed: int = 0) -> dict:
    arg_keys = jax.random.split(jax.random.key(seed), 6)
    north_vel = scatter_about(arg_keys[0], (MEMBERS, MONTHS, LEVELS, NLAT, NLON), 1.0, 6.0, ((0, 2), (3, 4), (4, 4)))
    up_vel = scatter_about(arg_keys[1], (MEMBERS, MONTHS, LEVELS, NLAT, NLON), 1.0, 6.0, ((0, 2), (3, 4), (4, 4)))
    dens_class = place_ends(jax.random.randint(arg_keys[2], (MEMBERS, MONTHS, LEVELS, NLAT, NLON), 0, CLASSES), jax.random.fold_in(arg_keys[2], 1), 0, CLASSES - 1).astype(jnp.int32)
    thickness = place_ends(jax.random.randint(arg_keys[3], (LEVELS, NLAT, NLON), 0, 2001), jax.random.fold_in(arg_keys[3], 1), 0, 2000).astype(jnp.int32)
    basin_id = place_ends(jax.random.randint(arg_keys[4], (NLAT, NLON), 0, BASINS + 1), jax.random.fold_in(arg_keys[4], 1), 0, BASINS).astype(jnp.int32)
    return {"north_vel": north_vel, "up_vel": up_vel, "dens_class": dens_class, "thickness": thickness, "basin_id": basin_id}


north_unit = 0.02
up_unit = 0.01

def class_sums(north_flux, rise_flux, dens_class, basin_masks):
    months, levels, lat_rows, lon_cells = north_flux.shape
    weighted = jnp.stack([north_flux, rise_flux], 2).reshape(months * levels, 2, lat_rows, lon_cells)
    classes_flat = dens_class.reshape(months * levels, lat_rows, lon_cells)
    class_ids = jnp.arange(CLASSES, dtype=jnp.int32)

    def one_level(packed):
        onehot = (packed[1][..., None] == class_ids).astype(jnp.float32)
        return jnp.einsum('sji,bji,jic->bscj', packed[0], basin_masks, onehot, precision=lax.Precision.HIGHEST)
    per_level = lax.map(one_level, (weighted, classes_flat))
    return lax.optimization_barrier(jnp.sum(per_level.reshape(months, levels, BASINS, 2, CLASSES, lat_rows), axis=1))

def member_tables(north_vel, up_vel, dens_class, thickness, basin_id, first_row, lat_total):
    months, levels, lat_rows, lon_cells = north_vel.shape
    row_index = first_row + jnp.arange(lat_rows, dtype=jnp.int32)
    latitude = (-78.0 + 156.0 * (row_index.astype(jnp.float32) + 0.5) / lat_total) * (math.pi / 180.0)
    zonal_width = jnp.cos(latitude)
    layer_depth = thickness.astype(jnp.float32) * 0.001
    wet_cells = (thickness > 0).astype(jnp.float32)
    north_flux = north_vel.astype(jnp.float32) * (north_unit * zonal_width)[None, None, :, None] * layer_depth[None]
    rise_flux = up_vel.astype(jnp.float32) * (up_unit * zonal_width)[None, None, :, None] * wet_cells[None]
    north_flux = north_flux.astype(jnp.bfloat16).astype(jnp.float32)
    rise_flux = rise_flux.astype(jnp.bfloat16).astype(jnp.float32)
    basin_masks = (basin_id[None] == jnp.arange(1, BASINS + 1, dtype=jnp.int32)[:, None, None]).astype(jnp.float32)
    north_depth = jnp.einsum('mkji,bji->mbkj', north_flux, basin_masks, precision=lax.Precision.HIGHEST)
    rise_depth = jnp.einsum('mkji,bji->mbkj', rise_flux, basin_masks, precision=lax.Precision.HIGHEST)
    depth_tab = jnp.stack([north_depth, rise_depth], 2)
    class_tab = class_sums(north_flux, rise_flux, dens_class, basin_masks)
    return (class_tab, depth_tab)

def with_global(tables):
    return jnp.concatenate([lax.optimization_barrier(jnp.sum(tables, axis=2, keepdims=True)), tables], 2)

def moments(stack_moc):
    members = stack_moc.shape[0]
    mean_val = lax.optimization_barrier(jnp.sum(stack_moc, 0)) / members
    spread_val = jnp.sqrt(lax.optimization_barrier(jnp.sum(jnp.square(stack_moc - mean_val), 0)) / (members - 1))
    return (mean_val, spread_val)

def reference(north_vel, up_vel, dens_class, thickness, basin_id):

    def one_member(packed):
        return member_tables(packed[0], packed[1], packed[2], thickness, basin_id, 0, NLAT)
    class_tab, depth_tab = lax.map(one_member, (north_vel, up_vel, dens_class))
    class_reg = with_global(class_tab)
    depth_reg = with_global(depth_tab)
    class_moc = jnp.stack([jnp.cumsum(class_reg[:, :, :, 0], axis=3), jnp.cumsum(jnp.cumsum(class_reg[:, :, :, 1], axis=4), axis=3)], 3)
    depth_moc = jnp.stack([jnp.cumsum(depth_reg[:, :, :, 0], axis=3), jnp.cumsum(depth_reg[:, :, :, 1], axis=4)], 3)
    depth_mean, depth_spread = moments(depth_moc)
    class_mean, class_spread = moments(class_moc)
    return (depth_mean, depth_spread, class_mean, class_spread)
```

```python
import math

import jax
import jax.numpy as jnp
from jax import lax
from jax.experimental import pallas as pl
from jax.experimental.pallas import tpu as pltpu
from jax.sharding import PartitionSpec as P

CLASSES = 80
BASINS = 3
REGIONS = BASINS + 1
LOW = 32
SUB = 8


north_unit = 0.02
up_unit = 0.01

F32, BF16, F8 = jnp.float32, jnp.bfloat16, jnp.float8_e4m3fn
NT = (((1,), (1,)), ((), ()))
NN = (((1,), (0,)), ((), ()))


def round_up(n, k):
    return -(-n // k) * k


def iota(shape, axis):
    return lax.broadcasted_iota(jnp.int32, shape, axis)


def split(x):
    high = x.astype(BF16)
    return high, (x - high.astype(F32)).astype(BF16)


def exact_dot(ones, x, dims, ones_first=True):
    high, low = split(x)
    if ones_first:
        return lax.dot_general(ones, high, dims, preferred_element_type=F32) + lax.dot_general(
            ones, low, dims, preferred_element_type=F32
        )
    return lax.dot_general(high, ones, dims, preferred_element_type=F32) + lax.dot_general(
        low, ones, dims, preferred_element_type=F32
    )


def sizes_of(levels, rows):
    return dict(
        levels=levels,
        rows=rows,
        highs=-(-BASINS * CLASSES // LOW),
        span=-(-CLASSES // LOW),
        deep=round_up(levels, 16),
        even=round_up(levels, 2),
        lanes=REGIONS * rows,
    )


def first_high(b):
    return b * CLASSES // LOW


def prepare(sz, basin, consts):
    base_ref, mask_ref, upto_class, upto_level, upto_row = consts
    rows, lanes = sz["rows"], sz["lanes"]
    lons = basin.shape[1]
    base_ref[...] = jnp.where(basin > 0, (basin - 1) * CLASSES, -LOW * 64)
    regions = [basin > 0] + [basin == r for r in range(1, REGIONS)]
    mask = jnp.concatenate([jnp.where(r, 1.0, 0.0) for r in regions], axis=0)
    group = iota((lanes, lons), 0) % rows // SUB
    mask_ref[...] = jnp.concatenate(
        [jnp.where(group == g, mask, 0.0) for g in range(rows // SUB)], axis=1
    ).astype(BF16)

    shape = upto_class.shape[1:]
    item = iota(shape, 1) // SUB
    part, half = item % LOW // 2, item % 2
    target = jnp.where(half == 0, part, jnp.where(part == 0, LOW // 2, LOW - part))
    sign = jnp.where((half == 1) & (part > 0), -1.0, 1.0)
    count = (half == 0) & (part == 0)

    def weight(m):
        beyond = jnp.where(count & (m > LOW // 2) & (m < LOW), 1.0, 0.0)
        return jnp.where(m == target, sign, 0.0) + beyond

    for b in range(BASINS):
        low = b * CLASSES - (first_high(b) + item // LOW) * LOW
        start, stop = jnp.maximum(low, 0), jnp.minimum(low + iota(shape, 0), LOW - 1) + 1
        upto_class[b] = jnp.where(stop > start, weight(start) - weight(stop), 0.0).astype(BF16)
    shape = upto_level.shape
    upto_level[...] = jnp.where(iota(shape, 1) <= iota(shape, 0), 1.0, 0.0).astype(BF16)
    shape = upto_row.shape
    a, b = iota(shape, 0), iota(shape, 1)
    upto_row[...] = jnp.where((a // rows == b // rows) & (a <= b), 1.0, 0.0).astype(BF16)


def month_tables(sz, north, up, dens, thick, coef, consts, work, put):
    base_ref, mask_ref, upto_class, upto_level, upto_row = consts
    flux, depth, step_high, step_low = work
    rows, highs, levels, lanes = sz["rows"], sz["highs"], sz["levels"], sz["lanes"]
    groups, even, span = rows // SUB, sz["even"], sz["span"]
    zero = jnp.zeros((2 * SUB, 128), BF16)
    width = LOW * SUB

    upper = iota((2 * SUB, 128), 0) >= SUB
    lane = iota((SUB, width), 1)
    own = iota((SUB, width), 0) == lane % SUB
    inner = lane >= 4 * SUB

    for pair in range(rows // (2 * SUB)):
        cells = slice(pair * 2 * SUB, (pair + 1) * 2 * SUB)
        lhs, rhs = ([], []), ([], [])
        kept = None
        for k in range(levels):
            depth_k = thick[k, cells, :].astype(F32)
            nf = north[k, cells, :].astype(F32) * (coef[0, cells, :] * depth_k)
            rf = up[k, cells, :].astype(F32) * (coef[1, cells, :] * jnp.minimum(depth_k, 1.0))
            if k % 2 == 1 or k == levels - 1:
                first = kept if k % 2 == 1 else (nf, rf)
                second = (nf, rf) if k % 2 == 1 else (jnp.zeros_like(nf),) * 2
                for s in range(2):
                    for half in range(2):
                        part = slice(half * SUB, (half + 1) * SUB)
                        flux[s, 2 * pair + half, pl.ds(k // 2 * 2 * SUB, 2 * SUB), :] = (
                            jnp.concatenate([first[s][part], second[s][part]], 0).astype(BF16)
                        )
            kept = (nf, rf)
            q = base_ref[cells, :] + dens[k, cells, :]
            qf, lo = q.astype(F32), (q & (LOW - 1)).astype(F32)
            for half in range(2):
                part = slice(half * SUB, (half + 1) * SUB)
                join = lambda x, y: jnp.concatenate([x[part], y[part]], 0).astype(BF16)
                at_least = join(qf, qf - LOW)
                ends = join(lo, (LOW - 1) - lo)
                top = jnp.where(join(jnp.full_like(lo, LOW), lo) >= BF16(LOW // 2), BF16(1), zero)
                parts = [top] + [jnp.minimum(ends, BF16(p)) for p in range(1, LOW // 2)]
                rhs[half].append(jnp.concatenate(parts, 0).astype(F8))
                hits = [at_least >= BF16(2 * LOW * p) for p in range(highs // 2)]
                nd, rd = join(nf, nf), join(rf, rf)
                lhs[half].append(
                    jnp.concatenate(
                        [jnp.where(h, nd, zero) for h in hits]
                        + [jnp.where(h, rd, zero) for h in hits],
                        0,
                    )
                )
        for half in range(2):
            sums = lax.dot_general(
                jnp.concatenate(lhs[half], 1),
                jnp.concatenate(rhs[half], 1),
                NT,
                preferred_element_type=F32,
            )
            for s in range(2):
                for h in range(highs):
                    at = (s * highs + h) * SUB
                    here = sums[at : at + SUB]
                    if h + 1 < highs:
                        here = here - sums[at + SUB : at + 2 * SUB]
                    here = jnp.where(own, here, 0.0)
                    back = jnp.concatenate(
                        [pltpu.roll(here[:, c : c + 128], 2 * SUB, 1) for c in range(0, width, 128)],
                        1,
                    )
                    first = back[:, :128]
                    turned = [jnp.where(inner[:, :128], first, 0.0)]
                    for c in range(128, width, 128):
                        turned.append(
                            jnp.where(
                                lane[:, :128] < 2 * SUB, back[:, c - 128 : c], back[:, c : c + 128]
                            )
                        )
                    here = here - jnp.concatenate(turned, 1)
                    row = (s * groups + 2 * pair + half) * SUB
                    high, low = split(here)
                    step_high[row : row + SUB, h * width : (h + 1) * width] = high
                    step_low[row : row + SUB, h * width : (h + 1) * width] = low

    found = []
    for b in range(BASINS):
        cols = slice(first_high(b) * width, (first_high(b) + span) * width)
        found.append(
            lax.dot_general(upto_class[b], step_high[:, cols], NT, preferred_element_type=F32)
            + lax.dot_general(upto_class[b], step_low[:, cols], NT, preferred_element_type=F32)
        )
    found = [sum(found[1:], found[0])] + found
    row_own = iota((SUB, lanes), 0) == iota((SUB, lanes), 1) % SUB
    for s in range(2):
        total = jnp.concatenate([x[:, s * rows : (s + 1) * rows] for x in found], 1)
        cols = jnp.concatenate([flux[s, g] for g in range(groups)], 1)
        seen = lax.dot_general(cols, mask_ref[...], NT, preferred_element_type=F32)
        seen = jnp.where(row_own[None], seen.reshape(even, SUB, lanes), 0.0)
        depth[0:even, :] = jnp.sum(seen, axis=1)
        if s == 0:
            put(0, total)
            put(2, exact_dot(upto_level[...], depth[...], NN))
        else:
            put(1, exact_dot(upto_row[...], total, NN, False))
            put(3, exact_dot(upto_row[...], depth[...], NN, False))


def table_rows(sz):
    return [0, CLASSES, 2 * CLASSES, 2 * CLASSES + sz["deep"], 2 * (CLASSES + sz["deep"])]


def const_shapes(sz, lons):
    rows, lanes = sz["rows"], sz["lanes"]
    return [
        pltpu.VMEM((rows, lons), jnp.int32),
        pltpu.VMEM((lanes, rows // SUB * lons), BF16),
        pltpu.VMEM((BASINS, CLASSES, sz["span"] * LOW * SUB), BF16),
        pltpu.VMEM((sz["deep"], sz["deep"]), BF16),
        pltpu.VMEM((lanes, lanes), BF16),
    ]


def work_shapes(sz, lons):
    rows = sz["rows"]
    steps = pltpu.VMEM((2 * rows, sz["highs"] * LOW * SUB), BF16)
    return [
        pltpu.VMEM((2, rows // SUB, sz["even"] * SUB, lons), BF16),
        pltpu.VMEM((sz["deep"], sz["lanes"]), F32),
        steps,
        steps,
    ]


def fused(sz, north_vel, up_vel, dens_class, thickness, basin_id):
    _, months, levels, rows, lons = north_vel.shape
    lanes, deep = sz["lanes"], sz["deep"]
    at = table_rows(sz)
    tall = at[-1]
    ends = CLASSES + deep
    devices, lats, members = (lax.axis_size(a) for a in ("lon", "lat", "mem"))
    assert months == devices
    far = [(de, dl) for dl in range(1, lats) for de in range(members)]

    def kernel(north_h, up_h, dens_h, thick_h, basin_h, final, *scratch):
        consts, work, rest = scratch[:5], scratch[5:9], scratch[9:]
        (north, up, dens, thick, basin, coef, tab, inbox, mine, membox, tail, tailbox) = rest[:12]
        in_sem, fix_sem, send, recv, msend, mrecv, tsend, trecv = rest[12:]
        me, lat, mem = (lax.axis_index(a) for a in ("lon", "lat", "mem"))

        def inputs(t):
            month = lax.rem(me + 1 + t, devices)
            return [
                pltpu.make_async_copy(h.at[0, month], v.at[t], in_sem.at[t, i])
                for i, (h, v) in enumerate(((north_h, north), (up_h, up), (dens_h, dens)))
            ]

        fixed = [
            pltpu.make_async_copy(basin_h, basin, fix_sem.at[0]),
            pltpu.make_async_copy(thick_h, thick, fix_sem.at[1]),
        ]
        for copy in fixed + inputs(0):
            copy.start()
        for t in range(1, devices):
            for copy in inputs(t):
                copy.start()

        barrier = pltpu.get_barrier_semaphore()
        peers = [{"lon": lax.rem(me + d, devices)} for d in range(1, devices)]
        peers += [
            {"lat": lax.rem(lat + dl, lats), "mem": lax.rem(mem + de, members)}
            for dl in range(lats)
            for de in range(members)
            if dl or de
        ]
        for peer in peers:
            pl.semaphore_signal(
                barrier, inc=1, device_id=peer, device_id_type=pl.DeviceIdType.MESH
            )

        index = lat * rows + iota((rows, lons), 0)
        latitude = (-78.0 + 156.0 * (index.astype(F32) + 0.5) / (rows * lats)) * (math.pi / 180.0)
        width = jnp.cos(latitude)
        coef[0] = (north_unit * 0.001) * width
        coef[1] = up_unit * width
        work[1][...] = jnp.zeros_like(work[1])
        fixed[0].wait()
        prepare(sz, basin[...], consts)
        fixed[1].wait()

        def table_copy(t):
            return pltpu.make_async_remote_copy(
                src_ref=tab.at[t],
                dst_ref=inbox.at[t],
                send_sem=send.at[t],
                recv_sem=recv.at[t],
                device_id={"lon": lax.rem(me + 1 + t, devices)},
                device_id_type=pl.DeviceIdType.MESH,
            )

        def one_month(t, carry):
            for copy in inputs(t):
                copy.wait()

            def put(i, x):
                tab[t, at[i] : at[i + 1], :] = x

            month_tables(
                sz, north.at[t], up.at[t], dens.at[t], thick, coef, consts, work, put
            )

            @pl.when(t == 0)
            def _():
                pl.semaphore_wait(barrier, len(peers))

            @pl.when(t < devices - 1)
            def _():
                table_copy(t).start()

            return carry

        lax.fori_loop(0, devices, one_month, 0)

        total = tab[devices - 1]
        for t in range(devices - 1):
            table_copy(t).wait_recv()
            total = total + inbox[t]
        mine[...] = total
        copies = [
            pltpu.make_async_remote_copy(
                src_ref=mine,
                dst_ref=membox.at[de - 1],
                send_sem=msend.at[de - 1],
                recv_sem=mrecv.at[de - 1],
                device_id={"mem": lax.rem(mem + de, members)},
                device_id_type=pl.DeviceIdType.MESH,
            )
            for de in range(1, members)
        ]
        for copy in copies:
            copy.start()

        pick = (iota((2 * SUB, lanes), 1) == iota((2 * SUB, lanes), 0) * rows + rows - 1)
        pick = jnp.where(pick, 1.0, 0.0).astype(BF16)
        rise = jnp.concatenate([mine[at[1] : at[2], :], mine[at[3] : at[4], :]], 0)
        high, low = split(rise)
        tail[...] = lax.dot_general(pick, high, NT, preferred_element_type=F32) + lax.dot_general(
            pick, low, NT, preferred_element_type=F32
        )
        tails = [
            pltpu.make_async_remote_copy(
                src_ref=tail,
                dst_ref=tailbox.at[i],
                send_sem=tsend.at[i],
                recv_sem=trecv.at[i],
                device_id={"lat": lax.rem(lat + dl, lats), "mem": lax.rem(mem + de, members)},
                device_id_type=pl.DeviceIdType.MESH,
            )
            for i, (de, dl) in enumerate(far)
        ]
        for copy in tails:
            copy.start()

        wide = (iota((2 * SUB, lanes), 1) // rows) == iota((2 * SUB, lanes), 0)
        wide = jnp.where(wide, 1.0, 0.0).astype(BF16)
        for copy in tails:
            copy.wait_recv()
        for copy in copies:
            copy.wait_recv()
        for de in range(members):
            whole = mine if de == 0 else membox.at[de - 1]
            south = jnp.zeros((2 * SUB, ends), F32)
            for i, (other, dl) in enumerate(far):
                if other == de:
                    south = south + jnp.where(lat >= dl, tailbox[i], 0.0)
            high, low = split(south)
            tn = (((0,), (0,)), ((), ()))
            carry = lax.dot_general(
                high, wide, tn, preferred_element_type=F32
            ) + lax.dot_general(low, wide, tn, preferred_element_type=F32)
            final[de, at[0] : at[1], :] = whole[at[0] : at[1], :]
            final[de, at[1] : at[2], :] = whole[at[1] : at[2], :] + carry[:CLASSES]
            final[de, at[2] : at[3], :] = whole[at[2] : at[3], :]
            final[de, at[3] : at[4], :] = whole[at[3] : at[4], :] + carry[CLASSES:]

        for t in range(devices - 1):
            table_copy(t).wait_send()
        for copy in copies + tails:
            copy.wait_send()

    slots = max(1, devices - 1)
    dma = pltpu.SemaphoreType.DMA
    return pl.pallas_call(
        kernel,
        out_shape=jax.ShapeDtypeStruct((members, tall, lanes), F32),
        in_specs=[pl.BlockSpec(memory_space=pl.ANY)] * 5,
        out_specs=pl.BlockSpec(memory_space=pltpu.VMEM),
        scratch_shapes=const_shapes(sz, lons)
        + work_shapes(sz, lons)
        + [
            pltpu.VMEM((months, levels, rows, lons), north_vel.dtype),
            pltpu.VMEM((months, levels, rows, lons), up_vel.dtype),
            pltpu.VMEM((months, levels, rows, lons), dens_class.dtype),
            pltpu.VMEM((levels, rows, lons), thickness.dtype),
            pltpu.VMEM((rows, lons), basin_id.dtype),
            pltpu.VMEM((2, rows, lons), F32),
            pltpu.VMEM((devices, tall, lanes), F32),
            pltpu.VMEM((slots, tall, lanes), F32),
            pltpu.VMEM((tall, lanes), F32),
            pltpu.VMEM((members - 1, tall, lanes), F32),
            pltpu.VMEM((2 * SUB, ends), F32),
            pltpu.VMEM((len(far), 2 * SUB, ends), F32),
            dma((devices, 3)),
            dma((2,)),
            dma((slots,)),
            dma((slots,)),
            dma((members - 1,)),
            dma((members - 1,)),
            dma((len(far),)),
            dma((len(far),)),
        ],
        compiler_params=pltpu.CompilerParams(
            collective_id=0, has_side_effects=True, vmem_limit_bytes=60 * 2**20
        ),
    )(north_vel, up_vel, dens_class, thickness, basin_id)


def moments(sz, final):
    members = final.shape[0]
    at, rows, levels, lanes = table_rows(sz), sz["rows"], sz["levels"], sz["lanes"]

    def kernel(final, o_dm, o_ds, o_cm, o_cs):
        for s in range(2):
            for i, count, o_mean, o_spread in ((s, CLASSES, o_cm, o_cs), (2 + s, levels, o_dm, o_ds)):
                part = [final[de, at[i] : at[i + 1], :] for de in range(members)]
                mean = sum(part[1:], part[0]) / members
                square = [jnp.square(x - mean) for x in part]
                spread = jnp.sqrt(sum(square[1:], square[0]) / (members - 1))
                for o, x in ((o_mean, mean), (o_spread, spread)):
                    pad = round_up(x.shape[0], 128) - x.shape[0]
                    x = jnp.concatenate([x, jnp.zeros((pad, lanes), F32)], 0).T
                    for r in range(REGIONS):
                        o[0, r, s] = x[r * rows : (r + 1) * rows, :count]

    out = lambda n: jax.ShapeDtypeStruct((1, REGIONS, 2, rows, n), F32)
    outs = pl.pallas_call(
        kernel,
        out_shape=[out(levels), out(levels), out(CLASSES), out(CLASSES)],
        in_specs=[pl.BlockSpec(memory_space=pltpu.VMEM)],
        out_specs=[pl.BlockSpec(memory_space=pltpu.VMEM)] * 4,
    )(final)
    return tuple(jnp.swapaxes(x, 3, 4) for x in outs)


def body(north_vel, up_vel, dens_class, thickness, basin_id):
    levels, rows = north_vel.shape[2:4]
    sz = sizes_of(levels, rows)
    return moments(sz, fused(sz, north_vel, up_vel, dens_class, thickness, basin_id))


def solution(mesh):
    in_specs = (
        P("mem", None, None, "lat", "lon"),
        P("mem", None, None, "lat", "lon"),
        P("mem", None, None, "lat", "lon"),
        P(None, "lat", "lon"),
        P("lat", "lon"),
    )
    out_specs = (P("lon", None, None, None, "lat"),) * 4
    return jax.shard_map(body, mesh=mesh, in_specs=in_specs, out_specs=out_specs, check_vma=False)
```

```python
import math

import jax
import jax.numpy as jnp
from jax import lax
from jax.experimental import pallas as pl
from jax.experimental.pallas import tpu as pltpu
from jax.sharding import PartitionSpec as P

CLASSES = 80
BASINS = 3
REGIONS = BASINS + 1
LOW = 32
SUB = 8


north_unit = 0.02
up_unit = 0.01

F32, BF16, F8 = jnp.float32, jnp.bfloat16, jnp.float8_e4m3fn
NT = (((1,), (1,)), ((), ()))
NN = (((1,), (0,)), ((), ()))


def round_up(n, k):
    return -(-n // k) * k


def iota(shape, axis):
    return lax.broadcasted_iota(jnp.int32, shape, axis)


def split(x):
    high = x.astype(BF16)
    return high, (x - high.astype(F32)).astype(BF16)


def exact_dot(ones, x, dims, ones_first=True):
    high, low = split(x)
    if ones_first:
        return lax.dot_general(ones, high, dims, preferred_element_type=F32) + lax.dot_general(
            ones, low, dims, preferred_element_type=F32
        )
    return lax.dot_general(high, ones, dims, preferred_element_type=F32) + lax.dot_general(
        low, ones, dims, preferred_element_type=F32
    )


def sizes_of(levels, rows):
    return dict(
        levels=levels,
        rows=rows,
        pairs=rows // (2 * SUB),
        highs=-(-BASINS * CLASSES // LOW),
        span=-(-CLASSES // LOW),
        even=round_up(levels, SUB),
        wide=round_up(max(levels, CLASSES), 128),
        lanes=REGIONS * rows,
    )


def first_high(b):
    return b * CLASSES // LOW


def prepare(sz, basin, consts):
    base_ref, mask_ref, upto_class, upto_level, upto_row = consts
    rows = sz["rows"]
    base_ref[...] = jnp.where(basin > 0, (basin - 1) * CLASSES, -LOW * 64)
    regions = [basin > 0] + [basin == r for r in range(1, REGIONS)]
    regions = [jnp.where(r, 1.0, 0.0) for r in regions]
    item = iota((REGIONS * 2 * SUB, basin.shape[1]), 0) % (2 * SUB) // SUB
    for pair in range(sz["pairs"]):
        cells = slice(pair * 2 * SUB, (pair + 1) * 2 * SUB)
        mask = jnp.concatenate([r[cells] for r in regions], axis=0)
        halves = [jnp.where(item == half, mask, 0.0) for half in range(2)]
        none = [jnp.zeros_like(mask)] * 2
        mask_ref[pair] = jnp.concatenate(
            [jnp.concatenate(halves + none, 1), jnp.concatenate(none + halves, 1)], 0
        ).astype(BF16)

    shape = upto_class.shape[1:]
    item = iota(shape, 1) // SUB
    part, half = item % LOW // 2, item % 2
    target = jnp.where(half == 0, part, jnp.where(part == 0, LOW // 2, LOW - part))
    sign = jnp.where((half == 1) & (part > 0), -1.0, 1.0)
    count = (half == 0) & (part == 0)

    def weight(m):
        beyond = jnp.where(count & (m > LOW // 2) & (m < LOW), 1.0, 0.0)
        return jnp.where(m == target, sign, 0.0) + beyond

    for b in range(BASINS):
        low = b * CLASSES - (first_high(b) + item // LOW) * LOW
        start, stop = jnp.maximum(low, 0), jnp.minimum(low + iota(shape, 0), LOW - 1) + 1
        upto_class[b] = jnp.where(stop > start, weight(start) - weight(stop), 0.0).astype(BF16)
    shape = upto_level.shape
    upto_level[...] = jnp.where(iota(shape, 0) <= iota(shape, 1), 1.0, 0.0).astype(BF16)
    shape = upto_row.shape
    a, b = iota(shape, 0), iota(shape, 1)
    upto_row[...] = jnp.where((a // rows == b // rows) & (b <= a), 1.0, 0.0).astype(BF16)


def gather_rows(blocks):
    row = iota(blocks[0].shape, 0)
    step = SUB // 2
    while step:
        low = row & step == 0
        joined = []
        for i in range(step):
            x, y = blocks[i], blocks[i + step]
            if step == SUB // 2:
                other = pltpu.roll(jnp.where(low, y, x), step, 0)
            else:
                other = jnp.where(low, pltpu.roll(x, SUB - step, 0), pltpu.roll(y, step, 0))
            joined.append(jnp.where(low, x, y) + other)
        blocks = joined
        step //= 2
    return blocks[0]


def pair_tables(sz, pair, north, up, dens, thick, coef, base_ref, mask_ref, flux, tab):
    highs, levels = sz["highs"], sz["levels"]
    zero = jnp.zeros((2 * SUB, 128), BF16)
    width = LOW * SUB
    own = iota((SUB, 128), 0) == iota((SUB, 128), 1) % SUB
    cells = pl.ds(pl.multiple_of(pair * 2 * SUB, 2 * SUB), 2 * SUB)

    lhs, rhs = ([], []), ([], [])
    kept = None
    for k in range(levels):
        depth_k = thick[k, cells, :].astype(F32)
        nf = north[k, cells, :].astype(F32) * (coef[0, cells, :] * depth_k)
        rf = up[k, cells, :].astype(F32) * (coef[1, cells, :] * jnp.minimum(depth_k, 1.0))
        if k % 2 == 1 or k == levels - 1:
            first = kept if k % 2 == 1 else (nf, rf)
            second = (nf, rf) if k % 2 == 1 else (jnp.zeros_like(nf),) * 2
            for s in range(2):
                for half in range(2):
                    part = slice(half * SUB, (half + 1) * SUB)
                    flux[2 * s + half, pl.ds(k // 2 * 2 * SUB, 2 * SUB), :] = jnp.concatenate(
                        [first[s][part], second[s][part]], 0
                    ).astype(BF16)
        kept = (nf, rf)
        q = base_ref[cells, :] + dens[k, cells, :]
        qf, lo = q.astype(F32), (q & (LOW - 1)).astype(F32)
        for half in range(2):
            part = slice(half * SUB, (half + 1) * SUB)
            join = lambda x, y: jnp.concatenate([x[part], y[part]], 0).astype(BF16)
            at_least = join(qf, qf - LOW)
            ends = join(lo, (LOW - 1) - lo)
            top = jnp.where(join(jnp.full_like(lo, LOW), lo) >= BF16(LOW // 2), BF16(1), zero)
            parts = [top] + [jnp.minimum(ends, BF16(p)) for p in range(1, LOW // 2)]
            rhs[half].append(jnp.concatenate(parts, 0).astype(F8))
            hits = [at_least >= BF16(2 * LOW * p) for p in range(highs // 2)]
            nd, rd = join(nf, nf), join(rf, rf)
            lhs[half].append(
                jnp.concatenate(
                    [jnp.where(h, nd, zero) for h in hits]
                    + [jnp.where(h, rd, zero) for h in hits],
                    0,
                )
            )
    sums = [
        lax.dot_general(
            jnp.concatenate(lhs[half], 1),
            jnp.concatenate(rhs[half], 1),
            NT,
            preferred_element_type=F32,
        )
        for half in range(2)
    ]
    seen = lax.dot_general(
        jnp.concatenate([flux[i] for i in range(4)], 1),
        mask_ref[pair],
        NT,
        preferred_element_type=F32,
    )

    def put(row, blocks):
        tab[row : row + SUB, :] = gather_rows([jnp.where(own, x, 0.0) for x in blocks])

    for half in range(2):
        for s in range(2):
            for c in range(width // 128):
                put(
                    class_row(half, s, c),
                    [
                        sums[half][(s * highs + h) * SUB :, c * 128 : (c + 1) * 128][:SUB]
                        for h in range(highs)
                    ],
                )
    for k in range(0, sz["even"], SUB):
        put(class_row(2, 0, 0) + k, [seen[(k + i) * SUB : (k + i + 1) * SUB] for i in range(SUB)])


def class_row(half, s, c):
    return ((half * 2 + s) * (LOW * SUB // 128) + c) * SUB


def table_rows(sz):
    return class_row(2, 0, 0) + sz["even"]


def kind_rows(sz, s, deep):
    at = (2 * s + deep) * sz["lanes"]
    return slice(at, at + sz["lanes"])


def month_sums(sz, total, consts, steps, mine):
    _, _, upto_class, upto_level, upto_row = consts
    rows, pairs, highs, span = sz["rows"], sz["pairs"], sz["highs"], sz["span"]
    width, wide = LOW * SUB, sz["wide"]
    row, lane = iota((SUB, 128), 0), iota((SUB, 128), 1)
    own = row == lane % SUB
    for pair in range(pairs):
        for s in range(2):
            exact = []
            for half in range(2):
                here, back = [], []
                for c in range(width // 128):
                    at = class_row(half, s, c)
                    x = total[pair][at : at + SUB]
                    x = x - jnp.where(row < highs - 1, pltpu.roll(x, SUB - 1, 0), 0.0)
                    here.append(x)
                    back.append(pltpu.roll(x, 2 * SUB, 1))
                for c in range(width // 128):
                    if c == 0:
                        turned = jnp.where(lane < 4 * SUB, 0.0, back[0])
                    else:
                        turned = jnp.where(lane < 2 * SUB, back[c - 1], back[c])
                    x = here[c] - turned
                    high = x.astype(BF16).astype(F32)
                    exact.append((high, x - high))
            for i in range(2):
                for h in range(highs):
                    for c in range(width // 128):
                        both = [exact[half * (width // 128) + c][i] for half in range(2)]
                        both = [
                            jnp.where(own, jnp.broadcast_to(x[h : h + 1], (SUB, 128)), 0.0)
                            for x in both
                        ]
                        at = (i * 2 + s) * rows + pair * 2 * SUB
                        steps[at : at + 2 * SUB, h * width + c * 128 : h * width + (c + 1) * 128] = (
                            jnp.concatenate(both, 0).astype(BF16)
                        )
    found = []
    for b in range(BASINS):
        cols = slice(first_high(b) * width, (first_high(b) + span) * width)
        x = lax.dot_general(steps[:, cols], upto_class[b], NT, preferred_element_type=F32)
        found.append(x[: 2 * rows] + x[2 * rows :])
    found = [sum(found[1:], found[0])] + found
    deep = []
    for pair in range(pairs):
        x = total[pair][class_row(2, 0, 0) :]
        deep.append(jnp.concatenate([x, jnp.zeros((wide - x.shape[0], 128), F32)], 0).T)
    for s in range(2):
        classes = jnp.concatenate([x[s * rows : (s + 1) * rows] for x in found], 0)
        levels = []
        for r in range(REGIONS):
            for pair in range(pairs):
                at = (s * REGIONS + r) * 2 * SUB
                levels.append(deep[pair][at : at + 2 * SUB])
        levels = jnp.concatenate(levels, 0)
        if s == 0:
            mine[kind_rows(sz, 0, 0), :] = classes
            mine[kind_rows(sz, 0, 1), :] = exact_dot(upto_level[...], levels, NN, False)
        else:
            mine[kind_rows(sz, 1, 0), :] = exact_dot(upto_row[...], classes, NN)
            mine[kind_rows(sz, 1, 1), :] = exact_dot(upto_row[...], levels, NN)


def const_shapes(sz, lons):
    lanes, wide = sz["lanes"], sz["wide"]
    return [
        pltpu.VMEM((sz["rows"], lons), jnp.int32),
        pltpu.VMEM((sz["pairs"], 2 * REGIONS * 2 * SUB, 4 * lons), BF16),
        pltpu.VMEM((BASINS, wide, sz["span"] * LOW * SUB), BF16),
        pltpu.VMEM((wide, wide), BF16),
        pltpu.VMEM((lanes, lanes), BF16),
    ]


def work_shapes(sz, lons):
    return [
        pltpu.VMEM((4, sz["even"] * SUB, lons), BF16),
        pltpu.VMEM((4 * sz["rows"], sz["highs"] * LOW * SUB), BF16),
    ]


def fused(sz, north_vel, up_vel, dens_class, thickness, basin_id):
    _, months, levels, rows, lons = north_vel.shape
    lanes, wide, pairs = sz["lanes"], sz["wide"], sz["pairs"]
    tall = 4 * lanes
    devices, lats, members = (lax.axis_size(a) for a in ("lon", "lat", "mem"))
    assert months == devices and sz["highs"] == SUB and lons == 128
    far = [(de, dl) for dl in range(1, lats) for de in range(members)]

    def kernel(north_h, up_h, dens_h, thick_h, basin_h, final, *scratch):
        consts, (flux, steps), rest = scratch[:5], scratch[5:7], scratch[7:]
        (north, up, dens, thick, basin, coef, tab, inbox, mine, membox, tail, tailbox, south) = rest[:13]
        in_sem, fix_sem, send, recv, msend, mrecv, tsend, trecv = rest[13:]
        me, lat, mem = (lax.axis_index(a) for a in ("lon", "lat", "mem"))

        def cells(pair):
            return pl.ds(pl.multiple_of(pair * 2 * SUB, 2 * SUB), 2 * SUB)

        def inputs(t, pair):
            month = lax.rem(me + 1 + t, devices)
            return [
                pltpu.make_async_copy(
                    h.at[0, month, :, cells(pair), :],
                    v.at[t, :, cells(pair), :],
                    in_sem.at[t, pair, i],
                )
                for i, (h, v) in enumerate(((north_h, north), (up_h, up), (dens_h, dens)))
            ]

        def layers(pair):
            return pltpu.make_async_copy(
                thick_h.at[:, cells(pair), :], thick.at[:, cells(pair), :], fix_sem.at[1 + pair]
            )

        fixed = pltpu.make_async_copy(basin_h, basin, fix_sem.at[0])
        fixed.start()
        for t in range(devices):
            for pair in range(pairs):
                for copy in ([layers(pair)] if t == 0 else []) + inputs(t, pair):
                    copy.start()

        barrier = pltpu.get_barrier_semaphore()
        peers = [{"lon": lax.rem(me + d, devices)} for d in range(1, devices)]
        peers += [
            {"lat": lax.rem(lat + dl, lats), "mem": lax.rem(mem + de, members)}
            for dl in range(lats)
            for de in range(members)
            if dl or de
        ]
        for peer in peers:
            pl.semaphore_signal(
                barrier, inc=1, device_id=peer, device_id_type=pl.DeviceIdType.MESH
            )

        index = lat * rows + iota((rows, lons), 0)
        latitude = (-78.0 + 156.0 * (index.astype(F32) + 0.5) / (rows * lats)) * (math.pi / 180.0)
        zonal = jnp.cos(latitude)
        coef[0] = (north_unit * 0.001) * zonal
        coef[1] = up_unit * zonal
        flux[:, levels * SUB :, :] = jnp.zeros_like(flux[:, levels * SUB :, :])
        south[...] = jnp.zeros_like(south)
        fixed.wait()
        prepare(sz, basin[...], consts)

        def table_copy(t, pair):
            return pltpu.make_async_remote_copy(
                src_ref=tab.at[t, pair],
                dst_ref=inbox.at[t, pair],
                send_sem=send.at[t, pair],
                recv_sem=recv.at[t, pair],
                device_id={"lon": lax.rem(me + 1 + t, devices)},
                device_id_type=pl.DeviceIdType.MESH,
            )

        def one_pair(i, carry):
            t, pair = i // pairs, lax.rem(i, pairs)

            @pl.when(t == 0)
            def _():
                layers(pair).wait()

            for copy in inputs(t, pair):
                copy.wait()
            pair_tables(
                sz,
                pair,
                north.at[t],
                up.at[t],
                dens.at[t],
                thick,
                coef,
                consts[0],
                consts[1],
                flux,
                tab.at[t, pair],
            )

            @pl.when(i == 0)
            def _():
                pl.semaphore_wait(barrier, len(peers))

            @pl.when(t < devices - 1)
            def _():
                table_copy(t, pair).start()

            return carry

        lax.fori_loop(0, devices * pairs, one_pair, 0)

        totals = []
        for pair in range(pairs):
            total = tab[devices - 1, pair]
            for t in range(devices - 1):
                table_copy(t, pair).wait_recv()
                total = total + inbox[t, pair]
            totals.append(total)
        month_sums(sz, totals, consts, steps, mine)
        copies = [
            pltpu.make_async_remote_copy(
                src_ref=mine,
                dst_ref=membox.at[de - 1],
                send_sem=msend.at[de - 1],
                recv_sem=mrecv.at[de - 1],
                device_id={"mem": lax.rem(mem + de, members)},
                device_id_type=pl.DeviceIdType.MESH,
            )
            for de in range(1, members)
        ]
        for copy in copies:
            copy.start()
        for deep in range(2):
            for r in range(REGIONS):
                at = kind_rows(sz, 1, deep).start + (r + 1) * rows - 1
                tail[deep * REGIONS + r : deep * REGIONS + r + 1, :] = mine[at : at + 1, :]

        def tail_copy(i, de, dl):
            return pltpu.make_async_remote_copy(
                src_ref=tail,
                dst_ref=tailbox.at[i],
                send_sem=tsend.at[i],
                recv_sem=trecv.at[i],
                device_id={"lat": lax.rem(lat + dl, lats), "mem": lax.rem(mem + de, members)},
                device_id_type=pl.DeviceIdType.MESH,
            )

        for i, (de, dl) in enumerate(far):

            @pl.when(lat + dl < lats)
            def _():
                tail_copy(i, de, dl).start()

        for i, (de, dl) in enumerate(far):

            @pl.when(lat >= dl)
            def _():
                tail_copy(i, de, dl).wait_recv()
                south[de] = south[de] + tailbox[i]

        for copy in copies:
            copy.wait_recv()
        for s in range(2):
            for deep in range(2):
                for r in range(REGIONS):
                    at = kind_rows(sz, s, deep).start + r * rows
                    part = []
                    for de in range(members):
                        whole = mine if de == 0 else membox.at[de - 1]
                        x = whole[at : at + rows, :]
                        if s == 1:
                            x = x + south[de, deep * REGIONS + r : deep * REGIONS + r + 1, :]
                        part.append(x)
                    mean = sum(part[1:], part[0]) / members
                    square = [jnp.square(x - mean) for x in part]
                    final[0, at : at + rows, :] = mean
                    final[1, at : at + rows, :] = jnp.sqrt(
                        sum(square[1:], square[0]) / (members - 1)
                    )

        for t in range(devices - 1):
            for pair in range(pairs):
                table_copy(t, pair).wait_send()
        for copy in copies:
            copy.wait_send()
        for i, (de, dl) in enumerate(far):

            @pl.when(lat + dl < lats)
            def _():
                tail_copy(i, de, dl).wait_send()

    slots = max(1, devices - 1)
    dma = pltpu.SemaphoreType.DMA
    table = (table_rows(sz), 128)
    tails = (2 * REGIONS, wide)
    return pl.pallas_call(
        kernel,
        out_shape=jax.ShapeDtypeStruct((2, tall, wide), F32),
        in_specs=[pl.BlockSpec(memory_space=pl.ANY)] * 5,
        out_specs=pl.BlockSpec(memory_space=pltpu.VMEM),
        scratch_shapes=const_shapes(sz, lons)
        + work_shapes(sz, lons)
        + [
            pltpu.VMEM((months, levels, rows, lons), north_vel.dtype),
            pltpu.VMEM((months, levels, rows, lons), up_vel.dtype),
            pltpu.VMEM((months, levels, rows, lons), dens_class.dtype),
            pltpu.VMEM((levels, rows, lons), thickness.dtype),
            pltpu.VMEM((rows, lons), basin_id.dtype),
            pltpu.VMEM((2, rows, lons), F32),
            pltpu.VMEM((devices, pairs) + table, F32),
            pltpu.VMEM((slots, pairs) + table, F32),
            pltpu.VMEM((tall, wide), F32),
            pltpu.VMEM((members - 1, tall, wide), F32),
            pltpu.VMEM(tails, F32),
            pltpu.VMEM((len(far),) + tails, F32),
            pltpu.VMEM((members,) + tails, F32),
            dma((devices, pairs, 3)),
            dma((1 + pairs,)),
            dma((slots, pairs)),
            dma((slots, pairs)),
            dma((members - 1,)),
            dma((members - 1,)),
            dma((len(far),)),
            dma((len(far),)),
        ],
        compiler_params=pltpu.CompilerParams(
            collective_id=0, has_side_effects=True, vmem_limit_bytes=60 * 2**20
        ),
    )(north_vel, up_vel, dens_class, thickness, basin_id)


def place(sz, final):
    rows, levels = sz["rows"], sz["levels"]

    def kernel(final, *outs):
        for s in range(2):
            for deep, count in ((1, levels), (0, CLASSES)):
                for i in range(2):
                    for r in range(REGIONS):
                        at = kind_rows(sz, s, deep).start + r * rows
                        o = outs[i + 2 * (1 - deep)]
                        o[0, r, s] = final[i, at : at + rows, :count]

    out = lambda n: jax.ShapeDtypeStruct((1, REGIONS, 2, rows, n), F32)
    outs = pl.pallas_call(
        kernel,
        out_shape=[out(levels), out(levels), out(CLASSES), out(CLASSES)],
        in_specs=[pl.BlockSpec(memory_space=pltpu.VMEM)],
        out_specs=[pl.BlockSpec(memory_space=pltpu.VMEM)] * 4,
    )(final)
    return tuple(jnp.swapaxes(x, 3, 4) for x in outs)


def body(north_vel, up_vel, dens_class, thickness, basin_id):
    levels, rows = north_vel.shape[2:4]
    sz = sizes_of(levels, rows)
    return place(sz, fused(sz, north_vel, up_vel, dens_class, thickness, basin_id))


def solution(mesh):
    in_specs = (
        P("mem", None, None, "lat", "lon"),
        P("mem", None, None, "lat", "lon"),
        P("mem", None, None, "lat", "lon"),
        P(None, "lat", "lon"),
        P("lat", "lon"),
    )
    out_specs = (P("lon", None, None, None, "lat"),) * 4
    return jax.shard_map(body, mesh=mesh, in_specs=in_specs, out_specs=out_specs, check_vma=False)
```

```python
import math

import jax
import jax.numpy as jnp
from jax import lax
from jax.experimental import pallas as pl
from jax.experimental.pallas import tpu as pltpu
from jax.sharding import PartitionSpec as P

CLASSES = 80
BASINS = 3
REGIONS = BASINS + 1
LOW = 32
SUB = 8


north_unit = 0.02
up_unit = 0.01

F32, BF16, F8 = jnp.float32, jnp.bfloat16, jnp.float8_e4m3fn
NT = (((1,), (1,)), ((), ()))
NN = (((1,), (0,)), ((), ()))


def round_up(n, k):
    return -(-n // k) * k


def iota(shape, axis):
    return lax.broadcasted_iota(jnp.int32, shape, axis)


def split(x):
    high = x.astype(BF16)
    return high, (x - high.astype(F32)).astype(BF16)


def exact_dot(ones, x, dims, ones_first=True):
    high, low = split(x)
    if ones_first:
        return lax.dot_general(ones, high, dims, preferred_element_type=F32) + lax.dot_general(
            ones, low, dims, preferred_element_type=F32
        )
    return lax.dot_general(high, ones, dims, preferred_element_type=F32) + lax.dot_general(
        low, ones, dims, preferred_element_type=F32
    )


def sizes_of(levels, rows):
    return dict(
        levels=levels,
        rows=rows,
        pairs=rows // (2 * SUB),
        highs=-(-BASINS * CLASSES // LOW),
        span=-(-CLASSES // LOW),
        even=round_up(levels, SUB),
        wide=round_up(max(levels, CLASSES), 128),
        lanes=REGIONS * rows,
    )


def first_high(b):
    return b * CLASSES // LOW


def prepare(sz, basin, consts):
    base_ref, mask_ref, upto_class, upto_level, upto_row = consts
    rows = sz["rows"]
    base_ref[...] = jnp.where(basin > 0, (basin - 1) * CLASSES, -LOW * 64)
    regions = [basin > 0] + [basin == r for r in range(1, REGIONS)]
    regions = [jnp.where(r, 1.0, 0.0) for r in regions]
    item = iota((REGIONS * 2 * SUB, basin.shape[1]), 0) % (2 * SUB) // SUB
    for pair in range(sz["pairs"]):
        cells = slice(pair * 2 * SUB, (pair + 1) * 2 * SUB)
        mask = jnp.concatenate([r[cells] for r in regions], axis=0)
        halves = [jnp.where(item == half, mask, 0.0) for half in range(2)]
        none = [jnp.zeros_like(mask)] * 2
        mask_ref[pair] = jnp.concatenate(
            [jnp.concatenate(halves + none, 1), jnp.concatenate(none + halves, 1)], 0
        ).astype(BF16)

    shape = upto_class.shape[1:]
    item = iota(shape, 0) // SUB
    part, half = item % LOW // 2, item % 2
    target = jnp.where(half == 0, part, jnp.where(part == 0, LOW // 2, LOW - part))
    sign = jnp.where((half == 1) & (part > 0), -1.0, 1.0)
    count = (half == 0) & (part == 0)

    def weight(m):
        beyond = jnp.where(count & (m > LOW // 2) & (m < LOW), 1.0, 0.0)
        return jnp.where(m == target, sign, 0.0) + beyond

    for b in range(BASINS):
        low = b * CLASSES - (first_high(b) + item // LOW) * LOW
        start, stop = jnp.maximum(low, 0), jnp.minimum(low + iota(shape, 1), LOW - 1) + 1
        upto_class[b] = jnp.where(stop > start, weight(start) - weight(stop), 0.0).astype(BF16)
    shape = upto_level.shape
    upto_level[...] = jnp.where(iota(shape, 0) <= iota(shape, 1), 1.0, 0.0).astype(BF16)
    shape = upto_row.shape
    a, b = iota(shape, 0), iota(shape, 1)
    upto_row[...] = jnp.where((a // rows == b // rows) & (b <= a), 1.0, 0.0).astype(BF16)


def gather_rows(blocks):
    row = iota(blocks[0].shape, 0)
    step = SUB // 2
    while step:
        low = row & step == 0
        joined = []
        for i in range(step):
            x, y = blocks[i], blocks[i + step]
            if step == SUB // 2:
                other = pltpu.roll(jnp.where(low, y, x), step, 0)
            else:
                other = jnp.where(low, pltpu.roll(x, SUB - step, 0), pltpu.roll(y, step, 0))
            joined.append(jnp.where(low, x, y) + other)
        blocks = joined
        step //= 2
    return blocks[0]


def pair_tables(sz, pair, north, up, dens, thick, coef, base_ref, mask_ref, flux, tab):
    highs, levels = sz["highs"], sz["levels"]
    zero = jnp.zeros((2 * SUB, 128), BF16)
    width = LOW * SUB
    own = iota((SUB, 128), 0) == iota((SUB, 128), 1) % SUB
    cells = pl.ds(pl.multiple_of(pair * 2 * SUB, 2 * SUB), 2 * SUB)

    lhs, rhs = ([], []), ([], [])
    kept = None
    for k in range(levels):
        depth_k = thick[k, cells, :].astype(F32)
        nf = north[k, cells, :].astype(F32) * (coef[0, cells, :] * depth_k)
        rf = up[k, cells, :].astype(F32) * (coef[1, cells, :] * jnp.minimum(depth_k, 1.0))
        if k % 2 == 1 or k == levels - 1:
            first = kept if k % 2 == 1 else (nf, rf)
            second = (nf, rf) if k % 2 == 1 else (jnp.zeros_like(nf),) * 2
            for s in range(2):
                for half in range(2):
                    part = slice(half * SUB, (half + 1) * SUB)
                    flux[2 * s + half, pl.ds(k // 2 * 2 * SUB, 2 * SUB), :] = jnp.concatenate(
                        [first[s][part], second[s][part]], 0
                    ).astype(BF16)
        kept = (nf, rf)
        q = base_ref[cells, :] + dens[k, cells, :]
        qf, lo = q.astype(F32), (q & (LOW - 1)).astype(F32)
        for half in range(2):
            part = slice(half * SUB, (half + 1) * SUB)
            join = lambda x, y: jnp.concatenate([x[part], y[part]], 0).astype(BF16)
            at_least = join(qf, qf - LOW)
            ends = join(lo, (LOW - 1) - lo)
            top = jnp.where(join(jnp.full_like(lo, LOW), lo) >= BF16(LOW // 2), BF16(1), zero)
            parts = [top] + [jnp.minimum(ends, BF16(p)) for p in range(1, LOW // 2)]
            rhs[half].append(jnp.concatenate(parts, 0).astype(F8))
            hits = [at_least >= BF16(2 * LOW * p) for p in range(highs // 2)]
            nd, rd = join(nf, nf), join(rf, rf)
            lhs[half].append(
                jnp.concatenate(
                    [jnp.where(h, nd, zero) for h in hits]
                    + [jnp.where(h, rd, zero) for h in hits],
                    0,
                )
            )
    sums = [
        lax.dot_general(
            jnp.concatenate(lhs[half], 1),
            jnp.concatenate(rhs[half], 1),
            NT,
            preferred_element_type=F32,
        )
        for half in range(2)
    ]
    seen = lax.dot_general(
        jnp.concatenate([flux[i] for i in range(4)], 1),
        mask_ref[pair],
        NT,
        preferred_element_type=F32,
    )

    def put(row, blocks):
        tab[row : row + SUB, :] = gather_rows([jnp.where(own, x, 0.0) for x in blocks])

    for half in range(2):
        for s in range(2):
            for c in range(width // 128):
                put(
                    class_row(half, s, c),
                    [
                        sums[half][(s * highs + h) * SUB :, c * 128 : (c + 1) * 128][:SUB]
                        for h in range(highs)
                    ],
                )
    for k in range(0, sz["even"], SUB):
        put(class_row(2, 0, 0) + k, [seen[(k + i) * SUB : (k + i + 1) * SUB] for i in range(SUB)])


def class_row(half, s, c):
    return ((half * 2 + s) * (LOW * SUB // 128) + c) * SUB


def table_rows(sz):
    return class_row(2, 0, 0) + sz["even"]


def kind_rows(sz, s, deep):
    at = (2 * s + deep) * sz["lanes"]
    return slice(at, at + sz["lanes"])


def month_sums(sz, total, consts, steps, mine, send_part):
    _, _, upto_class, upto_level, upto_row = consts
    rows, pairs, highs, span = sz["rows"], sz["pairs"], sz["highs"], sz["span"]
    width, wide = LOW * SUB, sz["wide"]
    row, lane = iota((SUB, 128), 0), iota((SUB, 128), 1)
    own = row == lane % SUB
    for pair in range(pairs):
        for s in range(2):
            exact = []
            for half in range(2):
                here, back = [], []
                for c in range(width // 128):
                    at = class_row(half, s, c)
                    x = total[pair][at : at + SUB]
                    x = x - jnp.where(row < highs - 1, pltpu.roll(x, SUB - 1, 0), 0.0)
                    here.append(x)
                    back.append(pltpu.roll(x, 2 * SUB, 1))
                for c in range(width // 128):
                    if c == 0:
                        turned = jnp.where(lane < 4 * SUB, 0.0, back[0])
                    else:
                        turned = jnp.where(lane < 2 * SUB, back[c - 1], back[c])
                    x = here[c] - turned
                    high = x.astype(BF16).astype(F32)
                    exact.append((high, x - high))
            for i in range(2):
                for h in range(highs):
                    for c in range(width // 128):
                        both = [exact[half * (width // 128) + c][i] for half in range(2)]
                        both = [
                            jnp.where(own, jnp.broadcast_to(x[h : h + 1], (SUB, 128)), 0.0)
                            for x in both
                        ]
                        at = (i * 2 + s) * rows + pair * 2 * SUB
                        steps[at : at + 2 * SUB, h * width + c * 128 : h * width + (c + 1) * 128] = (
                            jnp.concatenate(both, 0).astype(BF16)
                        )
    found = []
    for b in range(BASINS):
        cols = slice(first_high(b) * width, (first_high(b) + span) * width)
        x = lax.dot_general(steps[:, cols], upto_class[b], NN, preferred_element_type=F32)
        found.append(x[: 2 * rows] + x[2 * rows :])
    found = [sum(found[1:], found[0])] + found
    deep = []
    for pair in range(pairs):
        x = total[pair][class_row(2, 0, 0) :]
        deep.append(jnp.concatenate([x, jnp.zeros((wide - x.shape[0], 128), F32)], 0).T)
    for s in range(2):
        classes = jnp.concatenate([x[s * rows : (s + 1) * rows] for x in found], 0)
        levels = []
        for r in range(REGIONS):
            for pair in range(pairs):
                at = (s * REGIONS + r) * 2 * SUB
                levels.append(deep[pair][at : at + 2 * SUB])
        levels = jnp.concatenate(levels, 0)
        lanes = sz["lanes"]
        if s == 0:
            levels = exact_dot(upto_level[...], levels, NN, False)
        else:
            classes = exact_dot(upto_row[...], classes, NN)
            levels = exact_dot(upto_row[...], levels, NN)
        mine[s, :lanes, :] = classes
        mine[s, lanes:, :] = levels
        send_part(s)


def const_shapes(sz, lons):
    lanes, wide = sz["lanes"], sz["wide"]
    return [
        pltpu.VMEM((sz["rows"], lons), jnp.int32),
        pltpu.VMEM((sz["pairs"], 2 * REGIONS * 2 * SUB, 4 * lons), BF16),
        pltpu.VMEM((BASINS, sz["span"] * LOW * SUB, wide), BF16),
        pltpu.VMEM((wide, wide), BF16),
        pltpu.VMEM((lanes, lanes), BF16),
    ]


def work_shapes(sz, lons):
    return [
        pltpu.VMEM((4, sz["even"] * SUB, lons), BF16),
        pltpu.VMEM((4 * sz["rows"], sz["highs"] * LOW * SUB), BF16),
    ]


def fused(sz, north_vel, up_vel, dens_class, thickness, basin_id):
    _, months, levels, rows, lons = north_vel.shape
    lanes, wide, pairs = sz["lanes"], sz["wide"], sz["pairs"]
    tall = 4 * lanes
    devices, lats, members = (lax.axis_size(a) for a in ("lon", "lat", "mem"))
    assert months == devices and sz["highs"] == SUB and lons == 128
    far = [(de, dl) for dl in range(1, lats) for de in range(members)]

    def kernel(north_h, up_h, dens_h, thick_h, basin_h, final, *scratch):
        consts, (flux, steps), rest = scratch[:5], scratch[5:7], scratch[7:]
        (north, up, dens, thick, basin, coef, tab, inbox, mine, membox, tail, tailbox, south) = rest[:13]
        in_sem, fix_sem, send, recv, msend, mrecv, tsend, trecv = rest[13:]
        me, lat, mem = (lax.axis_index(a) for a in ("lon", "lat", "mem"))

        def cells(pair):
            return pl.ds(pl.multiple_of(pair * 2 * SUB, 2 * SUB), 2 * SUB)

        orders = [
            sorted((d for d in range(devices) if d != e), key=lambda d: (d != devices - 1 - e, d))
            for e in range(devices)
        ]

        def month_at(t):
            month = me
            for e, order in enumerate(orders):
                for turn, d in enumerate(order):
                    month = jnp.where((me == e) & (t == turn), d, month)
            return month

        def inputs(t, pair):
            month = month_at(t)
            return [
                pltpu.make_async_copy(
                    h.at[0, month, :, cells(pair), :],
                    v.at[t, :, cells(pair), :],
                    in_sem.at[t, pair, i],
                )
                for i, (h, v) in enumerate(((north_h, north), (up_h, up), (dens_h, dens)))
            ]

        def layers(pair):
            return pltpu.make_async_copy(
                thick_h.at[:, cells(pair), :], thick.at[:, cells(pair), :], fix_sem.at[1 + pair]
            )

        fixed = pltpu.make_async_copy(basin_h, basin, fix_sem.at[0])
        fixed.start()
        steps_ahead = min(2, devices * pairs)
        layers(0).start()
        for copy in inputs(0, 0):
            copy.start()

        barrier = pltpu.get_barrier_semaphore()
        peers = [{"lon": lax.rem(me + d, devices)} for d in range(1, devices)]
        peers += [
            {"lat": lax.rem(lat + dl, lats), "mem": lax.rem(mem + de, members)}
            for dl in range(lats)
            for de in range(members)
            if dl or de
        ]
        for peer in peers:
            pl.semaphore_signal(
                barrier, inc=1, device_id=peer, device_id_type=pl.DeviceIdType.MESH
            )

        index = lat * rows + iota((rows, lons), 0)
        latitude = (-78.0 + 156.0 * (index.astype(F32) + 0.5) / (rows * lats)) * (math.pi / 180.0)
        zonal = jnp.cos(latitude)
        coef[0] = (north_unit * 0.001) * zonal
        coef[1] = up_unit * zonal
        flux[:, levels * SUB :, :] = jnp.zeros_like(flux[:, levels * SUB :, :])
        south[...] = jnp.zeros_like(south)
        fixed.wait()
        prepare(sz, basin[...], consts)
        for i in range(1, steps_ahead):
            for copy in ([layers(i)] if i < pairs else []) + inputs(i // pairs, i % pairs):
                copy.start()

        def table_copy(t, pair):
            owner = month_at(t)
            slot = lax.rem(owner - me + devices, devices) - 1
            return pltpu.make_async_remote_copy(
                src_ref=tab.at[t, pair],
                dst_ref=inbox.at[slot, pair],
                send_sem=send.at[t, pair],
                recv_sem=recv.at[slot, pair],
                device_id={"lon": owner},
                device_id_type=pl.DeviceIdType.MESH,
            )

        def arrival(slot, pair):
            return pltpu.make_async_remote_copy(
                src_ref=tab.at[0, pair],
                dst_ref=inbox.at[slot, pair],
                send_sem=send.at[0, pair],
                recv_sem=recv.at[slot, pair],
                device_id={"lon": lax.rem(me + 1, devices)},
                device_id_type=pl.DeviceIdType.MESH,
            )

        hold = min(2, (devices - 1) * pairs - 1)

        def one_pair(i, carry):
            t, pair = i // pairs, lax.rem(i, pairs)

            @pl.when(i + steps_ahead < devices * pairs)
            def _():
                later = i + steps_ahead
                for copy in inputs(later // pairs, lax.rem(later, pairs)):
                    copy.start()

            if steps_ahead < pairs:

                @pl.when(i + steps_ahead < pairs)
                def _():
                    layers(i + steps_ahead).start()

            @pl.when(t == 0)
            def _():
                layers(pair).wait()

            for copy in inputs(t, pair):
                copy.wait()
            pair_tables(
                sz,
                pair,
                north.at[t],
                up.at[t],
                dens.at[t],
                thick,
                coef,
                consts[0],
                consts[1],
                flux,
                tab.at[t, pair],
            )

            @pl.when(i == hold)
            def _():
                pl.semaphore_wait(barrier, len(peers))
                for j in range(hold):
                    table_copy(j // pairs, j % pairs).start()

            @pl.when((i >= hold) & (t < devices - 1))
            def _():
                table_copy(t, pair).start()

            return carry

        lax.fori_loop(0, devices * pairs, one_pair, 0)

        totals = []
        for pair in range(pairs):
            total = tab[devices - 1, pair]
            for t in range(devices - 1):
                arrival(t, pair).wait_recv()
                total = total + inbox[t, pair]
            totals.append(total)
        copies = [
            [
                pltpu.make_async_remote_copy(
                    src_ref=mine.at[s],
                    dst_ref=membox.at[de - 1, s],
                    send_sem=msend.at[de - 1, s],
                    recv_sem=mrecv.at[de - 1, s],
                    device_id={"mem": lax.rem(mem + de, members)},
                    device_id_type=pl.DeviceIdType.MESH,
                )
                for de in range(1, members)
            ]
            for s in range(2)
        ]

        def send_part(s):
            for copy in copies[s]:
                copy.start()

        month_sums(sz, totals, consts, steps, mine, send_part)
        for deep in range(2):
            for r in range(REGIONS):
                at = deep * lanes + (r + 1) * rows - 1
                tail[deep * REGIONS + r : deep * REGIONS + r + 1, :] = mine[1, at : at + 1, :]

        def tail_copy(i, de, dl):
            return pltpu.make_async_remote_copy(
                src_ref=tail,
                dst_ref=tailbox.at[i],
                send_sem=tsend.at[i],
                recv_sem=trecv.at[i],
                device_id={"lat": lax.rem(lat + dl, lats), "mem": lax.rem(mem + de, members)},
                device_id_type=pl.DeviceIdType.MESH,
            )

        for i, (de, dl) in enumerate(far):

            @pl.when(lat + dl < lats)
            def _():
                tail_copy(i, de, dl).start()

        for s in range(2):
            if s == 1:
                for i, (de, dl) in enumerate(far):

                    @pl.when(lat >= dl)
                    def _():
                        tail_copy(i, de, dl).wait_recv()
                        south[de] = south[de] + tailbox[i]

            for copy in copies[s]:
                copy.wait_recv()
            for deep in range(2):
                for r in range(REGIONS):
                    at = deep * lanes + r * rows
                    part = []
                    for de in range(members):
                        whole = mine.at[s] if de == 0 else membox.at[de - 1, s]
                        x = whole[at : at + rows, :]
                        if s == 1:
                            x = x + south[de, deep * REGIONS + r : deep * REGIONS + r + 1, :]
                        part.append(x)
                    mean = sum(part[1:], part[0]) / members
                    square = [jnp.square(x - mean) for x in part]
                    at += s * 2 * lanes
                    final[0, at : at + rows, :] = mean
                    final[1, at : at + rows, :] = jnp.sqrt(
                        sum(square[1:], square[0]) / (members - 1)
                    )

        for t in range(devices - 1):
            for pair in range(pairs):
                table_copy(t, pair).wait_send()
        for copy in copies[0] + copies[1]:
            copy.wait_send()
        for i, (de, dl) in enumerate(far):

            @pl.when(lat + dl < lats)
            def _():
                tail_copy(i, de, dl).wait_send()

    arrays = (north_vel, up_vel, dens_class, thickness, basin_id)
    slots = max(1, devices - 1)
    dma = pltpu.SemaphoreType.DMA
    table = (table_rows(sz), 128)
    tails = (2 * REGIONS, wide)
    return pl.pallas_call(
        kernel,
        out_shape=jax.ShapeDtypeStruct((2, tall, wide), F32),
        in_specs=[pl.BlockSpec(memory_space=pl.ANY)] * 5,
        out_specs=pl.BlockSpec(memory_space=pltpu.VMEM),
        scratch_shapes=const_shapes(sz, lons)
        + work_shapes(sz, lons)
        + [
            pltpu.VMEM((months, levels, rows, lons), north_vel.dtype),
            pltpu.VMEM((months, levels, rows, lons), up_vel.dtype),
            pltpu.VMEM((months, levels, rows, lons), dens_class.dtype),
            pltpu.VMEM((levels, rows, lons), thickness.dtype),
            pltpu.VMEM((rows, lons), basin_id.dtype),
            pltpu.VMEM((2, rows, lons), F32),
            pltpu.VMEM((devices, pairs) + table, F32),
            pltpu.VMEM((slots, pairs) + table, F32),
            pltpu.VMEM((2, 2 * lanes, wide), F32),
            pltpu.VMEM((members - 1, 2, 2 * lanes, wide), F32),
            pltpu.VMEM(tails, F32),
            pltpu.VMEM((len(far),) + tails, F32),
            pltpu.VMEM((members,) + tails, F32),
            dma((devices, pairs, 3)),
            dma((1 + pairs,)),
            dma((slots, pairs)),
            dma((slots, pairs)),
            dma((members - 1, 2)),
            dma((members - 1, 2)),
            dma((len(far),)),
            dma((len(far),)),
        ],
        compiler_params=pltpu.CompilerParams(
            collective_id=0, has_side_effects=True, vmem_limit_bytes=44 * 2**20
        ),
    )(*[pltpu.with_memory_space_constraint(x, pltpu.HBM) for x in arrays])


def place(sz, final):
    rows, levels = sz["rows"], sz["levels"]

    def kernel(final, *outs):
        for s in range(2):
            for deep, count in ((1, levels), (0, CLASSES)):
                for i in range(2):
                    for r in range(REGIONS):
                        at = kind_rows(sz, s, deep).start + r * rows
                        o = outs[i + 2 * (1 - deep)]
                        o[0, r, s] = final[i, at : at + rows, :count]

    out = lambda n: jax.ShapeDtypeStruct((1, REGIONS, 2, rows, n), F32)
    outs = pl.pallas_call(
        kernel,
        out_shape=[out(levels), out(levels), out(CLASSES), out(CLASSES)],
        in_specs=[pl.BlockSpec(memory_space=pltpu.VMEM)],
        out_specs=[pl.BlockSpec(memory_space=pltpu.VMEM)] * 4,
        compiler_params=pltpu.CompilerParams(vmem_limit_bytes=8 * 2**20),
    )(final)
    return tuple(jnp.swapaxes(x, 3, 4) for x in outs)


def body(north_vel, up_vel, dens_class, thickness, basin_id):
    levels, rows = north_vel.shape[2:4]
    sz = sizes_of(levels, rows)
    return place(sz, fused(sz, north_vel, up_vel, dens_class, thickness, basin_id))


def solution(mesh):
    in_specs = (
        P("mem", None, None, "lat", "lon"),
        P("mem", None, None, "lat", "lon"),
        P("mem", None, None, "lat", "lon"),
        P(None, "lat", "lon"),
        P("lat", "lon"),
    )
    out_specs = (P("lon", None, None, None, "lat"),) * 4
    return jax.shard_map(body, mesh=mesh, in_specs=in_specs, out_specs=out_specs, check_vma=False)
```

```python
import math

import jax
import jax.numpy as jnp
from jax import lax
from jax.experimental import pallas as pl
from jax.experimental.pallas import tpu as pltpu
from jax.sharding import PartitionSpec as P

CLASSES = 80
BASINS = 3
REGIONS = BASINS + 1
LOW = 32
SUB = 8


north_unit = 0.02
up_unit = 0.01

F32, BF16, F8 = jnp.float32, jnp.bfloat16, jnp.float8_e4m3fn
NT = (((1,), (1,)), ((), ()))
NN = (((1,), (0,)), ((), ()))


def round_up(n, k):
    return -(-n // k) * k


def iota(shape, axis):
    return lax.broadcasted_iota(jnp.int32, shape, axis)


def split(x):
    high = x.astype(BF16)
    return high, (x - high.astype(F32)).astype(BF16)


def exact_dot(ones, x, dims, ones_first=True):
    high, low = split(x)
    if ones_first:
        return lax.dot_general(ones, high, dims, preferred_element_type=F32) + lax.dot_general(
            ones, low, dims, preferred_element_type=F32
        )
    return lax.dot_general(high, ones, dims, preferred_element_type=F32) + lax.dot_general(
        low, ones, dims, preferred_element_type=F32
    )


def sizes_of(levels, rows):
    return dict(
        levels=levels,
        rows=rows,
        pairs=rows // (2 * SUB),
        highs=-(-BASINS * CLASSES // LOW),
        span=-(-CLASSES // LOW),
        near=round_up(-(-levels // 2), 2),
        wide=round_up(max(levels, CLASSES), 128),
        lanes=REGIONS * rows,
    )


def first_high(b):
    return b * CLASSES // LOW


def prepare_weights(sz, consts):
    _, _, upto_class, upto_level, upto_row = consts
    rows = sz["rows"]
    wide = upto_class.shape[2]
    c = iota((SUB, wide), 1)
    for b in range(BASINS):
        for h in range(sz["span"]):
            low = b * CLASSES - (first_high(b) + h) * LOW
            start = max(low, 0)
            stop = jnp.minimum(c + (low + 1), LOW)
            some = stop > start
            beyond = some & (stop > LOW // 2) & (stop < LOW)
            for part in range(LOW // 2):
                both = []
                for half in range(2):
                    target = part if half == 0 else (LOW - part if part else LOW // 2)
                    sign = -1.0 if half == 1 and part else 1.0
                    first = sign if start == target else 0.0
                    x = jnp.where(some, first - jnp.where(stop == target, sign, 0.0), 0.0)
                    if half == 0 and part == 0:
                        if LOW // 2 < start < LOW:
                            x = x + jnp.where(some, 1.0, 0.0)
                        x = x - jnp.where(beyond, 1.0, 0.0)
                    both.append(x)
                at = (h * LOW + 2 * part) * SUB
                upto_class[b, at : at + 2 * SUB, :] = jnp.concatenate(both, 0).astype(BF16)
    shape = upto_level.shape
    upto_level[...] = jnp.where(iota(shape, 0) <= iota(shape, 1), 1.0, 0.0).astype(BF16)
    shape = upto_row.shape
    a, b = iota(shape, 0), iota(shape, 1)
    upto_row[...] = jnp.where((a // rows == b // rows) & (b <= a), 1.0, 0.0).astype(BF16)


def prepare_masks(sz, basin, consts):
    base_ref, mask_ref = consts[:2]
    lons = basin.shape[1]
    base_ref[...] = jnp.where(basin > 0, (basin - 1) * CLASSES, -LOW * 64)
    regions = [basin > 0] + [basin == r for r in range(1, REGIONS)]
    regions = [jnp.where(r, 1.0, 0.0) for r in regions]
    lane = iota((lons, 2 * REGIONS * 2 * SUB), 1)
    none = jnp.zeros(lane.shape, BF16)
    for pair in range(sz["pairs"]):
        cells = slice(pair * 2 * SUB, (pair + 1) * 2 * SUB)
        mask = jnp.concatenate([r[cells] for r in regions] * 2, axis=0).T
        for s in range(2):
            for half in range(2):
                here = (lane // (REGIONS * 2 * SUB) == s) & (lane // SUB % 2 == half)
                here = jnp.where(here, mask, 0.0).astype(BF16)
                for late in range(2):
                    at = (late * 4 + 2 * s + half) * lons
                    mask_ref[pair, at : at + lons, :] = jnp.concatenate(
                        [none, here] if late else [here, none], 1
                    )


def gather_rows(blocks):
    row = iota(blocks[0].shape, 0)
    step = SUB // 2
    while step:
        low = row & step == 0
        joined = []
        for i in range(step):
            x, y = blocks[i], blocks[i + step]
            if step == SUB // 2:
                other = pltpu.roll(jnp.where(low, y, x), step, 0)
            else:
                other = jnp.where(low, pltpu.roll(x, SUB - step, 0), pltpu.roll(y, step, 0))
            joined.append(jnp.where(low, x, y) + other)
        blocks = joined
        step //= 2
    return blocks[0]


def pair_tables(sz, pair, north, up, dens, thick, coef, base_ref, mask_ref, flux, tab):
    highs, levels = sz["highs"], sz["levels"]
    zero = jnp.zeros((2 * SUB, 128), BF16)
    width = LOW * SUB
    own = iota((SUB, 128), 0) == iota((SUB, 128), 1) % SUB
    cells = pl.ds(pl.multiple_of(pair * 2 * SUB, 2 * SUB), 2 * SUB)

    lhs, rhs = ([], []), ([], [])
    kept = None
    for k in range(levels):
        depth_k = thick[k, cells, :].astype(F32)
        nf = north[k, cells, :].astype(F32) * (coef[0, cells, :] * depth_k)
        rf = up[k, cells, :].astype(F32) * (coef[1, cells, :] * jnp.minimum(depth_k, 1.0))
        if k % 2 == 1 or k == levels - 1:
            first = kept if k % 2 == 1 else (nf, rf)
            second = (nf, rf) if k % 2 == 1 else (jnp.zeros_like(nf),) * 2
            for s in range(2):
                for half in range(2):
                    part = slice(half * SUB, (half + 1) * SUB)
                    flux[2 * s + half, pl.ds(k // 2 * 2 * SUB, 2 * SUB), :] = jnp.concatenate(
                        [first[s][part], second[s][part]], 0
                    ).astype(BF16)
        kept = (nf, rf)
        q = base_ref[cells, :] + dens[k, cells, :]
        qf, lo = q.astype(F32), (q & (LOW - 1)).astype(F32)
        for half in range(2):
            part = slice(half * SUB, (half + 1) * SUB)
            join = lambda x, y: jnp.concatenate([x[part], y[part]], 0).astype(BF16)
            at_least = join(qf, qf - LOW)
            ends = join(lo, (LOW - 1) - lo)
            top = jnp.where(join(jnp.full_like(lo, LOW), lo) >= BF16(LOW // 2), BF16(1), zero)
            parts = [top] + [jnp.minimum(ends, BF16(p)) for p in range(1, LOW // 2)]
            rhs[half].append(jnp.concatenate(parts, 0).astype(F8))
            hits = [at_least >= BF16(2 * LOW * p) for p in range(highs // 2)]
            nd, rd = join(nf, nf), join(rf, rf)
            lhs[half].append(
                jnp.concatenate(
                    [jnp.where(h, nd, zero) for h in hits]
                    + [jnp.where(h, rd, zero) for h in hits],
                    0,
                )
            )
    sums = [
        lax.dot_general(
            jnp.concatenate(lhs[half], 1),
            jnp.concatenate(rhs[half], 1),
            NT,
            preferred_element_type=F32,
        )
        for half in range(2)
    ]
    near = sz["near"] * SUB
    seen = lax.dot_general(
        jnp.concatenate([flux[i, late * near : (late + 1) * near, :] for late in range(2) for i in range(4)], 1),
        mask_ref[pair],
        NN,
        preferred_element_type=F32,
    )

    def put(row, blocks):
        tab[row : row + SUB, :] = gather_rows([jnp.where(own, x, 0.0) for x in blocks])

    for half in range(2):
        for s in range(2):
            for c in range(width // 128):
                put(
                    class_row(half, s, c),
                    [
                        sums[half][(s * highs + h) * SUB :, c * 128 : (c + 1) * 128][:SUB]
                        for h in range(highs)
                    ],
                )

    def level(k):
        if k >= levels:
            return jnp.zeros((SUB, 128), F32)
        late, k = divmod(k, sz["near"])
        return seen[k * SUB : (k + 1) * SUB, late * 128 : (late + 1) * 128]

    for k in range(0, levels, SUB):
        put(class_row(2, 0, 0) + k, [level(k + i) for i in range(SUB)])


def class_row(half, s, c):
    return ((half * 2 + s) * (LOW * SUB // 128) + c) * SUB


def table_rows(sz):
    return class_row(2, 0, 0) + round_up(sz["levels"], SUB)


def kind_rows(sz, s, deep):
    at = (2 * s + deep) * sz["lanes"]
    return slice(at, at + sz["lanes"])


def month_sums(sz, total, consts, steps, mine, send_tail, send_part):
    _, _, upto_class, upto_level, upto_row = consts
    rows, pairs, highs, span = sz["rows"], sz["pairs"], sz["highs"], sz["span"]
    width, wide = LOW * SUB, sz["wide"]
    row, lane = iota((SUB, 128), 0), iota((SUB, 128), 1)
    own = row == lane % SUB
    for pair in range(pairs):
        for s in range(2):
            exact = []
            for half in range(2):
                here, back = [], []
                for c in range(width // 128):
                    at = class_row(half, s, c)
                    x = total[pair][at : at + SUB]
                    x = x - jnp.where(row < highs - 1, pltpu.roll(x, SUB - 1, 0), 0.0)
                    here.append(x)
                    back.append(pltpu.roll(x, 2 * SUB, 1))
                for c in range(width // 128):
                    if c == 0:
                        turned = jnp.where(lane < 4 * SUB, 0.0, back[0])
                    else:
                        turned = jnp.where(lane < 2 * SUB, back[c - 1], back[c])
                    x = here[c] - turned
                    high = x.astype(BF16).astype(F32)
                    exact.append((high, x - high))
            for i in range(2):
                for h in range(highs):
                    for c in range(width // 128):
                        both = [exact[half * (width // 128) + c][i] for half in range(2)]
                        both = [
                            jnp.where(own, jnp.broadcast_to(x[h : h + 1], (SUB, 128)), 0.0)
                            for x in both
                        ]
                        at = (i * 2 + s) * rows + pair * 2 * SUB
                        steps[at : at + 2 * SUB, h * width + c * 128 : h * width + (c + 1) * 128] = (
                            jnp.concatenate(both, 0).astype(BF16)
                        )
    found = []
    for b in range(BASINS):
        cols = slice(first_high(b) * width, (first_high(b) + span) * width)
        x = lax.dot_general(steps[:, cols], upto_class[b], NN, preferred_element_type=F32)
        found.append(x[: 2 * rows] + x[2 * rows :])
    found = [sum(found[1:], found[0])] + found
    deep = []
    for pair in range(pairs):
        x = total[pair][class_row(2, 0, 0) :]
        deep.append(jnp.concatenate([x, jnp.zeros((wide - x.shape[0], 128), F32)], 0).T)
    tables = []
    for s in range(2):
        classes = jnp.concatenate([x[s * rows : (s + 1) * rows] for x in found], 0)
        levels = []
        for r in range(REGIONS):
            for pair in range(pairs):
                at = (s * REGIONS + r) * 2 * SUB
                levels.append(deep[pair][at : at + 2 * SUB])
        tables.append((classes, jnp.concatenate(levels, 0)))
    send_tail(
        [
            jnp.sum(x[r * rows : (r + 1) * rows], axis=0, keepdims=True)
            for x in tables[1]
            for r in range(REGIONS)
        ]
    )
    lanes = sz["lanes"]
    for s in range(2):
        classes, levels = tables[s]
        if s == 0:
            levels = exact_dot(upto_level[...], levels, NN, False)
        else:
            classes = exact_dot(upto_row[...], classes, NN)
            levels = exact_dot(upto_row[...], levels, NN)
        mine[s, :lanes, :] = classes
        mine[s, lanes:, :] = levels
        send_part(s)


def const_shapes(sz, lons):
    lanes, wide = sz["lanes"], sz["wide"]
    return [
        pltpu.VMEM((sz["rows"], lons), jnp.int32),
        pltpu.VMEM((sz["pairs"], 8 * lons, 2 * 2 * REGIONS * 2 * SUB), BF16),
        pltpu.VMEM((BASINS, sz["span"] * LOW * SUB, wide), BF16),
        pltpu.VMEM((wide, wide), BF16),
        pltpu.VMEM((lanes, lanes), BF16),
    ]


def work_shapes(sz, lons):
    return [
        pltpu.VMEM((4, 2 * sz["near"] * SUB, lons), BF16),
        pltpu.VMEM((4 * sz["rows"], sz["highs"] * LOW * SUB), BF16),
    ]


def fused(sz, north_vel, up_vel, dens_class, thickness, basin_id):
    _, months, levels, rows, lons = north_vel.shape
    lanes, wide, pairs = sz["lanes"], sz["wide"], sz["pairs"]
    tall = 4 * lanes
    devices, lats, members = (lax.axis_size(a) for a in ("lon", "lat", "mem"))
    assert months == devices and sz["highs"] == SUB and lons == 128
    far = [(de, dl) for dl in range(1, lats) for de in range(members)]

    def kernel(north_h, up_h, dens_h, thick_h, basin_h, final, *scratch):
        consts, (flux, steps), rest = scratch[:5], scratch[5:7], scratch[7:]
        (north, up, dens, thick, basin, coef, tab, inbox, mine, membox, tail, tailbox, south) = rest[:13]
        in_sem, fix_sem, send, recv, msend, mrecv, tsend, trecv = rest[13:]
        me, lat, mem = (lax.axis_index(a) for a in ("lon", "lat", "mem"))

        def cells(pair):
            return pl.ds(pl.multiple_of(pair * 2 * SUB, 2 * SUB), 2 * SUB)

        orders = [
            sorted((d for d in range(devices) if d != e), key=lambda d: (d != devices - 1 - e, d))
            for e in range(devices)
        ]

        def month_at(t):
            month = me
            for e, order in enumerate(orders):
                for turn, d in enumerate(order):
                    month = jnp.where((me == e) & (t == turn), d, month)
            return month

        def inputs(t, pair):
            month = month_at(t)
            return [
                pltpu.make_async_copy(
                    h.at[0, month, :, cells(pair), :],
                    v.at[t, :, cells(pair), :],
                    in_sem.at[t, pair, i],
                )
                for i, (h, v) in enumerate(((north_h, north), (up_h, up), (dens_h, dens)))
            ]

        def layers(pair):
            return pltpu.make_async_copy(
                thick_h.at[:, cells(pair), :], thick.at[:, cells(pair), :], fix_sem.at[1 + pair]
            )

        fixed = pltpu.make_async_copy(basin_h, basin, fix_sem.at[0])
        fixed.start()
        steps_ahead = min(2, devices * pairs)
        layers(0).start()
        for copy in inputs(0, 0):
            copy.start()

        barrier = pltpu.get_barrier_semaphore()
        peers = [{"lon": lax.rem(me + d, devices)} for d in range(1, devices)]
        peers += [
            {"lat": lax.rem(lat + dl, lats), "mem": lax.rem(mem + de, members)}
            for dl in range(lats)
            for de in range(members)
            if dl or de
        ]
        for peer in peers:
            pl.semaphore_signal(
                barrier, inc=1, device_id=peer, device_id_type=pl.DeviceIdType.MESH
            )

        index = lat * rows + iota((rows, lons), 0)
        latitude = (-78.0 + 156.0 * (index.astype(F32) + 0.5) / (rows * lats)) * (math.pi / 180.0)
        zonal = jnp.cos(latitude)
        coef[0] = (north_unit * 0.001) * zonal
        coef[1] = up_unit * zonal
        flux[:, levels * SUB :, :] = jnp.zeros_like(flux[:, levels * SUB :, :])
        south[...] = jnp.zeros_like(south)
        prepare_weights(sz, consts)
        fixed.wait()
        prepare_masks(sz, basin[...], consts)
        for i in range(1, steps_ahead):
            for copy in ([layers(i)] if i < pairs else []) + inputs(i // pairs, i % pairs):
                copy.start()

        def table_copy(t, pair):
            owner = month_at(t)
            slot = lax.rem(owner - me + devices, devices) - 1
            return pltpu.make_async_remote_copy(
                src_ref=tab.at[t, pair],
                dst_ref=inbox.at[slot, pair],
                send_sem=send.at[t, pair],
                recv_sem=recv.at[slot, pair],
                device_id={"lon": owner},
                device_id_type=pl.DeviceIdType.MESH,
            )

        def arrival(slot, pair):
            return pltpu.make_async_remote_copy(
                src_ref=tab.at[0, pair],
                dst_ref=inbox.at[slot, pair],
                send_sem=send.at[0, pair],
                recv_sem=recv.at[slot, pair],
                device_id={"lon": lax.rem(me + 1, devices)},
                device_id_type=pl.DeviceIdType.MESH,
            )

        hold = min(1, (devices - 1) * pairs - 1)

        def one_pair(i, carry):
            t, pair = i // pairs, lax.rem(i, pairs)

            @pl.when(i + steps_ahead < devices * pairs)
            def _():
                later = i + steps_ahead
                for copy in inputs(later // pairs, lax.rem(later, pairs)):
                    copy.start()

            if steps_ahead < pairs:

                @pl.when(i + steps_ahead < pairs)
                def _():
                    layers(i + steps_ahead).start()

            @pl.when(t == 0)
            def _():
                layers(pair).wait()

            for copy in inputs(t, pair):
                copy.wait()
            pair_tables(
                sz,
                pair,
                north.at[t],
                up.at[t],
                dens.at[t],
                thick,
                coef,
                consts[0],
                consts[1],
                flux,
                tab.at[t, pair],
            )

            @pl.when(i == hold)
            def _():
                pl.semaphore_wait(barrier, len(peers))
                for j in range(hold):
                    table_copy(j // pairs, j % pairs).start()

            @pl.when((i >= hold) & (t < devices - 1))
            def _():
                table_copy(t, pair).start()

            return carry

        lax.fori_loop(0, devices * pairs, one_pair, 0)

        totals = []
        for pair in range(pairs):
            total = tab[devices - 1, pair]
            for t in range(devices - 1):
                arrival(t, pair).wait_recv()
                total = total + inbox[t, pair]
            totals.append(total)
        copies = [
            [
                pltpu.make_async_remote_copy(
                    src_ref=mine.at[s],
                    dst_ref=membox.at[de - 1, s],
                    send_sem=msend.at[de - 1, s],
                    recv_sem=mrecv.at[de - 1, s],
                    device_id={"mem": lax.rem(mem + de, members)},
                    device_id_type=pl.DeviceIdType.MESH,
                )
                for de in range(1, members)
            ]
            for s in range(2)
        ]

        def send_part(s):
            for copy in copies[s]:
                copy.start()

        def tail_copy(i, de, dl):
            return pltpu.make_async_remote_copy(
                src_ref=tail,
                dst_ref=tailbox.at[i],
                send_sem=tsend.at[i],
                recv_sem=trecv.at[i],
                device_id={"lat": lax.rem(lat + dl, lats), "mem": lax.rem(mem + de, members)},
                device_id_type=pl.DeviceIdType.MESH,
            )

        def send_tail(lines):
            for r, line in enumerate(lines):
                tail[r : r + 1, :] = line
            for i, (de, dl) in enumerate(far):

                @pl.when(lat + dl < lats)
                def _():
                    tail_copy(i, de, dl).start()

        month_sums(sz, totals, consts, steps, mine, send_tail, send_part)
        for s in range(2):
            if s == 1:
                for i, (de, dl) in enumerate(far):

                    @pl.when(lat >= dl)
                    def _():
                        tail_copy(i, de, dl).wait_recv()
                        south[de] = south[de] + tailbox[i]

            for copy in copies[s]:
                copy.wait_recv()
            for deep in range(2):
                for r in range(REGIONS):
                    at = deep * lanes + r * rows
                    part = []
                    for de in range(members):
                        whole = mine.at[s] if de == 0 else membox.at[de - 1, s]
                        x = whole[at : at + rows, :]
                        if s == 1:
                            x = x + south[de, deep * REGIONS + r : deep * REGIONS + r + 1, :]
                        part.append(x)
                    mean = sum(part[1:], part[0]) / members
                    square = [jnp.square(x - mean) for x in part]
                    at += s * 2 * lanes
                    final[0, at : at + rows, :] = mean
                    final[1, at : at + rows, :] = jnp.sqrt(
                        sum(square[1:], square[0]) / (members - 1)
                    )

        for t in range(devices - 1):
            for pair in range(pairs):
                table_copy(t, pair).wait_send()
        for copy in copies[0] + copies[1]:
            copy.wait_send()
        for i, (de, dl) in enumerate(far):

            @pl.when(lat + dl < lats)
            def _():
                tail_copy(i, de, dl).wait_send()

    arrays = (north_vel, up_vel, dens_class, thickness, basin_id)
    slots = max(1, devices - 1)
    dma = pltpu.SemaphoreType.DMA
    table = (table_rows(sz), 128)
    tails = (2 * REGIONS, wide)
    return pl.pallas_call(
        kernel,
        out_shape=jax.ShapeDtypeStruct((2, tall, wide), F32),
        in_specs=[pl.BlockSpec(memory_space=pl.ANY)] * 5,
        out_specs=pl.BlockSpec(memory_space=pltpu.VMEM),
        scratch_shapes=const_shapes(sz, lons)
        + work_shapes(sz, lons)
        + [
            pltpu.VMEM((months, levels, rows, lons), north_vel.dtype),
            pltpu.VMEM((months, levels, rows, lons), up_vel.dtype),
            pltpu.VMEM((months, levels, rows, lons), dens_class.dtype),
            pltpu.VMEM((levels, rows, lons), thickness.dtype),
            pltpu.VMEM((rows, lons), basin_id.dtype),
            pltpu.VMEM((2, rows, lons), F32),
            pltpu.VMEM((devices, pairs) + table, F32),
            pltpu.VMEM((slots, pairs) + table, F32),
            pltpu.VMEM((2, 2 * lanes, wide), F32),
            pltpu.VMEM((members - 1, 2, 2 * lanes, wide), F32),
            pltpu.VMEM(tails, F32),
            pltpu.VMEM((len(far),) + tails, F32),
            pltpu.VMEM((members,) + tails, F32),
            dma((devices, pairs, 3)),
            dma((1 + pairs,)),
            dma((slots, pairs)),
            dma((slots, pairs)),
            dma((members - 1, 2)),
            dma((members - 1, 2)),
            dma((len(far),)),
            dma((len(far),)),
        ],
        compiler_params=pltpu.CompilerParams(
            collective_id=0, has_side_effects=True, vmem_limit_bytes=44 * 2**20
        ),
    )(*[pltpu.with_memory_space_constraint(x, pltpu.HBM) for x in arrays])


def place(sz, final):
    rows, levels = sz["rows"], sz["levels"]

    def kernel(final, *outs):
        for s in range(2):
            for deep, count in ((1, levels), (0, CLASSES)):
                for i in range(2):
                    for r in range(REGIONS):
                        at = kind_rows(sz, s, deep).start + r * rows
                        o = outs[i + 2 * (1 - deep)]
                        o[0, r, s] = final[i, at : at + rows, :count]

    out = lambda n: jax.ShapeDtypeStruct((1, REGIONS, 2, rows, n), F32)
    outs = pl.pallas_call(
        kernel,
        out_shape=[out(levels), out(levels), out(CLASSES), out(CLASSES)],
        in_specs=[pl.BlockSpec(memory_space=pltpu.VMEM)],
        out_specs=[pl.BlockSpec(memory_space=pltpu.VMEM)] * 4,
        compiler_params=pltpu.CompilerParams(vmem_limit_bytes=8 * 2**20),
    )(final)
    return tuple(jnp.swapaxes(x, 3, 4) for x in outs)


def body(north_vel, up_vel, dens_class, thickness, basin_id):
    levels, rows = north_vel.shape[2:4]
    sz = sizes_of(levels, rows)
    return place(sz, fused(sz, north_vel, up_vel, dens_class, thickness, basin_id))


def solution(mesh):
    in_specs = (
        P("mem", None, None, "lat", "lon"),
        P("mem", None, None, "lat", "lon"),
        P("mem", None, None, "lat", "lon"),
        P(None, "lat", "lon"),
        P("lat", "lon"),
    )
    out_specs = (P("lon", None, None, None, "lat"),) * 4
    return jax.shard_map(body, mesh=mesh, in_specs=in_specs, out_specs=out_specs, check_vma=False)
```

```python
import math

import jax
import jax.numpy as jnp
from jax import lax
from jax.experimental import pallas as pl
from jax.experimental.pallas import tpu as pltpu
from jax.sharding import PartitionSpec as P

CLASSES = 80
BASINS = 3
REGIONS = BASINS + 1
LOW = 32
SUB = 8


north_unit = 0.02
up_unit = 0.01

F32, BF16, F8 = jnp.float32, jnp.bfloat16, jnp.float8_e4m3fn
NT = (((1,), (1,)), ((), ()))
NN = (((1,), (0,)), ((), ()))


def round_up(n, k):
    return -(-n // k) * k


def iota(shape, axis):
    return lax.broadcasted_iota(jnp.int32, shape, axis)


def split(x):
    high = x.astype(BF16)
    return high, (x - high.astype(F32)).astype(BF16)


def exact_dot(ones, x, dims, ones_first=True):
    high, low = split(x)
    if ones_first:
        return lax.dot_general(ones, high, dims, preferred_element_type=F32) + lax.dot_general(
            ones, low, dims, preferred_element_type=F32
        )
    return lax.dot_general(high, ones, dims, preferred_element_type=F32) + lax.dot_general(
        low, ones, dims, preferred_element_type=F32
    )


def sizes_of(levels, rows):
    return dict(
        levels=levels,
        rows=rows,
        pairs=rows // (2 * SUB),
        highs=-(-BASINS * CLASSES // LOW),
        span=-(-CLASSES // LOW),
        near=round_up(-(-levels // 2), 2),
        wide=round_up(max(levels, CLASSES), 128),
        lanes=REGIONS * rows,
    )


def first_high(b):
    return b * CLASSES // LOW


def prepare_weights(sz, consts):
    _, _, upto_class, upto_level, upto_row = consts
    rows = sz["rows"]
    wide = upto_class.shape[2]
    c = iota((SUB, wide), 1)
    for b in range(BASINS):
        for h in range(sz["span"]):
            low = b * CLASSES - (first_high(b) + h) * LOW
            start = max(low, 0)
            stop = jnp.minimum(c + (low + 1), LOW)
            some = stop > start
            beyond = some & (stop > LOW // 2) & (stop < LOW)
            for part in range(LOW // 2):
                both = []
                for half in range(2):
                    target = part if half == 0 else (LOW - part if part else LOW // 2)
                    sign = -1.0 if half == 1 and part else 1.0
                    first = sign if start == target else 0.0
                    x = jnp.where(some, first - jnp.where(stop == target, sign, 0.0), 0.0)
                    if half == 0 and part == 0:
                        if LOW // 2 < start < LOW:
                            x = x + jnp.where(some, 1.0, 0.0)
                        x = x - jnp.where(beyond, 1.0, 0.0)
                    both.append(x)
                at = (h * LOW + 2 * part) * SUB
                upto_class[b, at : at + 2 * SUB, :] = jnp.concatenate(both, 0).astype(BF16)
    shape = upto_level.shape
    upto_level[...] = jnp.where(iota(shape, 0) <= iota(shape, 1), 1.0, 0.0).astype(BF16)
    shape = upto_row.shape
    a, b = iota(shape, 0), iota(shape, 1)
    upto_row[...] = jnp.where((a // rows == b // rows) & (b <= a), 1.0, 0.0).astype(BF16)


def prepare_masks(sz, basin, consts):
    base_ref, mask_ref = consts[:2]
    lons = basin.shape[1]
    base_ref[...] = jnp.where(basin > 0, (basin - 1) * CLASSES, -LOW * 64)
    regions = [basin > 0] + [basin == r for r in range(1, REGIONS)]
    regions = [jnp.where(r, 1.0, 0.0) for r in regions]
    lane = iota((lons, 2 * REGIONS * 2 * SUB), 1)
    none = jnp.zeros(lane.shape, BF16)
    for pair in range(sz["pairs"]):
        cells = slice(pair * 2 * SUB, (pair + 1) * 2 * SUB)
        mask = jnp.concatenate([r[cells] for r in regions] * 2, axis=0).T
        for s in range(2):
            for half in range(2):
                here = (lane // (REGIONS * 2 * SUB) == s) & (lane // SUB % 2 == half)
                here = jnp.where(here, mask, 0.0).astype(BF16)
                for late in range(2):
                    at = (late * 4 + 2 * s + half) * lons
                    mask_ref[pair, at : at + lons, :] = jnp.concatenate(
                        [none, here] if late else [here, none], 1
                    )


def gather_rows(blocks):
    row = iota(blocks[0].shape, 0)
    step = SUB // 2
    while step:
        low = row & step == 0
        joined = []
        for i in range(step):
            x, y = blocks[i], blocks[i + step]
            if step == SUB // 2:
                other = pltpu.roll(jnp.where(low, y, x), step, 0)
            else:
                other = jnp.where(low, pltpu.roll(x, SUB - step, 0), pltpu.roll(y, step, 0))
            joined.append(jnp.where(low, x, y) + other)
        blocks = joined
        step //= 2
    return blocks[0]


def pair_tables(sz, pair, north, up, dens, thick, coef, base_ref, mask_ref, flux, tab):
    highs, levels = sz["highs"], sz["levels"]
    zero = jnp.zeros((2 * SUB, 128), BF16)
    width = LOW * SUB
    own = iota((SUB, 128), 0) == iota((SUB, 128), 1) % SUB
    start = pair * 2 * SUB
    cells = pl.ds(start if isinstance(pair, int) else pl.multiple_of(start, 2 * SUB), 2 * SUB)

    lhs, rhs = ([], []), ([], [])
    kept = None
    for k in range(levels):
        depth_k = thick[k, cells, :].astype(F32)
        nf = north[k, cells, :].astype(F32) * (coef[0, cells, :] * depth_k)
        rf = up[k, cells, :].astype(F32) * (coef[1, cells, :] * jnp.minimum(depth_k, 1.0))
        if k % 2 == 1 or k == levels - 1:
            first = kept if k % 2 == 1 else (nf, rf)
            second = (nf, rf) if k % 2 == 1 else (jnp.zeros_like(nf),) * 2
            for s in range(2):
                for half in range(2):
                    part = slice(half * SUB, (half + 1) * SUB)
                    flux[2 * s + half, pl.ds(k // 2 * 2 * SUB, 2 * SUB), :] = jnp.concatenate(
                        [first[s][part], second[s][part]], 0
                    ).astype(BF16)
        kept = (nf, rf)
        q = base_ref[cells, :] + dens[k, cells, :]
        qf, lo = q.astype(F32), (q & (LOW - 1)).astype(F32)
        for half in range(2):
            part = slice(half * SUB, (half + 1) * SUB)
            join = lambda x, y: jnp.concatenate([x[part], y[part]], 0).astype(BF16)
            at_least = join(qf, qf - LOW)
            ends = join(lo, (LOW - 1) - lo)
            top = jnp.where(join(jnp.full_like(lo, LOW), lo) >= BF16(LOW // 2), BF16(1), zero)
            parts = [top] + [jnp.minimum(ends, BF16(p)) for p in range(1, LOW // 2)]
            rhs[half].append(jnp.concatenate(parts, 0).astype(F8))
            hits = [at_least >= BF16(2 * LOW * p) for p in range(highs // 2)]
            nd, rd = join(nf, nf), join(rf, rf)
            lhs[half].append(
                jnp.concatenate(
                    [jnp.where(h, nd, zero) for h in hits]
                    + [jnp.where(h, rd, zero) for h in hits],
                    0,
                )
            )
    sums = [
        lax.dot_general(
            jnp.concatenate(lhs[half], 1),
            jnp.concatenate(rhs[half], 1),
            NT,
            preferred_element_type=F32,
        )
        for half in range(2)
    ]
    near = sz["near"] * SUB
    seen = lax.dot_general(
        jnp.concatenate([flux[i, late * near : (late + 1) * near, :] for late in range(2) for i in range(4)], 1),
        mask_ref[pair],
        NN,
        preferred_element_type=F32,
    )

    def put(row, blocks):
        tab[row : row + SUB, :] = gather_rows([jnp.where(own, x, 0.0) for x in blocks])

    for half in range(2):
        for s in range(2):
            for c in range(width // 128):
                put(
                    class_row(half, s, c),
                    [
                        sums[half][(s * highs + h) * SUB :, c * 128 : (c + 1) * 128][:SUB]
                        for h in range(highs)
                    ],
                )

    def level(k):
        if k >= levels:
            return jnp.zeros((SUB, 128), F32)
        late, k = divmod(k, sz["near"])
        return seen[k * SUB : (k + 1) * SUB, late * 128 : (late + 1) * 128]

    for k in range(0, levels, SUB):
        put(class_row(2, 0, 0) + k, [level(k + i) for i in range(SUB)])


def class_row(half, s, c):
    return ((half * 2 + s) * (LOW * SUB // 128) + c) * SUB


def table_rows(sz):
    return class_row(2, 0, 0) + round_up(sz["levels"], SUB)


def kind_rows(sz, s, deep):
    at = (2 * s + deep) * sz["lanes"]
    return slice(at, at + sz["lanes"])


def month_sums(sz, total, consts, steps, mine, send_tail, send_part):
    _, _, upto_class, upto_level, upto_row = consts
    rows, pairs, highs, span = sz["rows"], sz["pairs"], sz["highs"], sz["span"]
    width, wide = LOW * SUB, sz["wide"]
    row, lane = iota((SUB, 128), 0), iota((SUB, 128), 1)
    own = row == lane % SUB
    for pair in range(pairs):
        for s in range(2):
            exact = []
            for half in range(2):
                here, back = [], []
                for c in range(width // 128):
                    at = class_row(half, s, c)
                    x = total[pair][at : at + SUB]
                    x = x - jnp.where(row < highs - 1, pltpu.roll(x, SUB - 1, 0), 0.0)
                    here.append(x)
                    back.append(pltpu.roll(x, 2 * SUB, 1))
                for c in range(width // 128):
                    if c == 0:
                        turned = jnp.where(lane < 4 * SUB, 0.0, back[0])
                    else:
                        turned = jnp.where(lane < 2 * SUB, back[c - 1], back[c])
                    x = here[c] - turned
                    high = x.astype(BF16).astype(F32)
                    exact.append((high, x - high))
            for i in range(2):
                for h in range(highs):
                    for c in range(width // 128):
                        both = [exact[half * (width // 128) + c][i] for half in range(2)]
                        both = [
                            jnp.where(own, jnp.broadcast_to(x[h : h + 1], (SUB, 128)), 0.0)
                            for x in both
                        ]
                        at = (i * 2 + s) * rows + pair * 2 * SUB
                        steps[at : at + 2 * SUB, h * width + c * 128 : h * width + (c + 1) * 128] = (
                            jnp.concatenate(both, 0).astype(BF16)
                        )
    found = []
    for b in range(BASINS):
        cols = slice(first_high(b) * width, (first_high(b) + span) * width)
        x = lax.dot_general(steps[:, cols], upto_class[b], NN, preferred_element_type=F32)
        found.append(x[: 2 * rows] + x[2 * rows :])
    found = [sum(found[1:], found[0])] + found
    deep = []
    for pair in range(pairs):
        x = total[pair][class_row(2, 0, 0) :]
        deep.append(jnp.concatenate([x, jnp.zeros((wide - x.shape[0], 128), F32)], 0).T)
    tables = []
    for s in range(2):
        classes = jnp.concatenate([x[s * rows : (s + 1) * rows] for x in found], 0)
        levels = []
        for r in range(REGIONS):
            for pair in range(pairs):
                at = (s * REGIONS + r) * 2 * SUB
                levels.append(deep[pair][at : at + 2 * SUB])
        tables.append((classes, jnp.concatenate(levels, 0)))
    send_tail(
        [
            jnp.sum(x[r * rows : (r + 1) * rows], axis=0, keepdims=True)
            for x in tables[1]
            for r in range(REGIONS)
        ]
    )
    lanes = sz["lanes"]
    done = [
        (tables[0][0], exact_dot(upto_level[...], tables[0][1], NN, False)),
        tuple(exact_dot(upto_row[...], x, NN) for x in tables[1]),
    ]
    for s in range(2):
        mine[s, :lanes, :], mine[s, lanes:, :] = done[s]
    for s in range(2):
        send_part(s)


def const_shapes(sz, lons):
    lanes, wide = sz["lanes"], sz["wide"]
    return [
        pltpu.VMEM((sz["rows"], lons), jnp.int32),
        pltpu.VMEM((sz["pairs"], 8 * lons, 2 * 2 * REGIONS * 2 * SUB), BF16),
        pltpu.VMEM((BASINS, sz["span"] * LOW * SUB, wide), BF16),
        pltpu.VMEM((wide, wide), BF16),
        pltpu.VMEM((lanes, lanes), BF16),
    ]


def work_shapes(sz, lons):
    return [
        pltpu.VMEM((sz["pairs"], 4, 2 * sz["near"] * SUB, lons), BF16),
        pltpu.VMEM((4 * sz["rows"], sz["highs"] * LOW * SUB), BF16),
    ]


def fused(sz, north_vel, up_vel, dens_class, thickness, basin_id):
    _, months, levels, rows, lons = north_vel.shape
    lanes, wide, pairs = sz["lanes"], sz["wide"], sz["pairs"]
    tall = 4 * lanes
    devices, lats, members = (lax.axis_size(a) for a in ("lon", "lat", "mem"))
    assert months == devices and sz["highs"] == SUB and lons == 128
    far = (lats - 1) * members

    def kernel(north_h, up_h, dens_h, thick_h, basin_h, final, *scratch):
        consts, (flux, steps), rest = scratch[:5], scratch[5:7], scratch[7:]
        (north, up, dens, thick, basin, coef, tab, inbox, mine, membox, tail, tailbox, south) = rest[:13]
        in_sem, fix_sem, send, recv, msend, mrecv, tsend, trecv = rest[13:]
        me, lat, mem = (lax.axis_index(a) for a in ("lon", "lat", "mem"))

        def cells(pair):
            return pl.ds(pl.multiple_of(pair * 2 * SUB, 2 * SUB), 2 * SUB)

        orders = [
            sorted((d for d in range(devices) if d != e), key=lambda d: (d != devices - 1 - e, d))
            for e in range(devices)
        ]

        def month_at(t):
            month = me
            for e, order in enumerate(orders):
                for turn, d in enumerate(order):
                    month = jnp.where((me == e) & (t == turn), d, month)
            return month

        def inputs(t, pair):
            month = month_at(t)
            return [
                pltpu.make_async_copy(
                    h.at[0, month, :, cells(pair), :],
                    v.at[t, :, cells(pair), :],
                    in_sem.at[t, pair, i],
                )
                for i, (h, v) in enumerate(((north_h, north), (up_h, up), (dens_h, dens)))
            ]

        def layers(pair):
            return pltpu.make_async_copy(
                thick_h.at[:, cells(pair), :], thick.at[:, cells(pair), :], fix_sem.at[1 + pair]
            )

        fixed = pltpu.make_async_copy(basin_h, basin, fix_sem.at[0])
        fixed.start()
        layers(0).start()
        for copy in inputs(0, 0):
            copy.start()

        barrier = pltpu.get_barrier_semaphore()
        peers = [{"lon": lax.rem(me + d, devices)} for d in range(1, devices)]
        peers += [
            {"lat": lax.rem(lat + dl, lats), "mem": lax.rem(mem + de, members)}
            for dl in range(lats)
            for de in range(members)
            if dl or de
        ]
        for peer in peers:
            pl.semaphore_signal(
                barrier, inc=1, device_id=peer, device_id_type=pl.DeviceIdType.MESH
            )

        index = lat * rows + iota((rows, lons), 0)
        latitude = (-78.0 + 156.0 * (index.astype(F32) + 0.5) / (rows * lats)) * (math.pi / 180.0)
        zonal = jnp.cos(latitude)
        coef[0] = (north_unit * 0.001) * zonal
        coef[1] = up_unit * zonal
        flux[:, :, levels * SUB :, :] = jnp.zeros_like(flux[:, :, levels * SUB :, :])
        south[...] = jnp.zeros_like(south)
        prepare_weights(sz, consts)
        fixed.wait()
        prepare_masks(sz, basin[...], consts)
        for pair in range(1, pairs):
            for copy in [layers(pair)] + inputs(0, pair):
                copy.start()

        def table_copy(t, pair):
            owner = month_at(t)
            slot = lax.rem(owner - me + devices, devices) - 1
            return pltpu.make_async_remote_copy(
                src_ref=tab.at[t, pair],
                dst_ref=inbox.at[slot, pair],
                send_sem=send.at[t, pair],
                recv_sem=recv.at[slot, pair],
                device_id={"lon": owner},
                device_id_type=pl.DeviceIdType.MESH,
            )

        def arrival(slot, pair):
            return pltpu.make_async_remote_copy(
                src_ref=tab.at[0, pair],
                dst_ref=inbox.at[slot, pair],
                send_sem=send.at[0, pair],
                recv_sem=recv.at[slot, pair],
                device_id={"lon": lax.rem(me + 1, devices)},
                device_id_type=pl.DeviceIdType.MESH,
            )


        def tables_of(t, pair):
            pair_tables(
                sz,
                pair,
                north.at[t],
                up.at[t],
                dens.at[t],
                thick,
                coef,
                consts[0],
                consts[1],
                flux.at[pair],
                tab.at[t, pair],
            )

        def one_month(t, carry):
            @pl.when(t + 1 < devices)
            def _():
                for pair in range(pairs):
                    for copy in inputs(t + 1, pair):
                        copy.start()

            stepwise = (lax.rem(t, 2) == 0) & (t < devices - 1)

            @pl.when(stepwise)
            def _():
                def one_pair(pair, carry):
                    @pl.when(t == 0)
                    def _():
                        layers(pair).wait()

                    for copy in inputs(t, pair):
                        copy.wait()
                    tables_of(t, pair)

                    @pl.when((t == 0) & (pair == pairs - 1))
                    def _():
                        pl.semaphore_wait(barrier, len(peers))
                        for j in range(pairs - 1):
                            table_copy(t, j).start()

                    @pl.when((t > 0) | (pair == pairs - 1))
                    def _():
                        table_copy(t, pair).start()

                    return carry

                lax.fori_loop(0, pairs, one_pair, 0)

            @pl.when(jnp.logical_not(stepwise))
            def _():
                for pair in range(pairs):
                    for copy in inputs(t, pair):
                        copy.wait()
                for pair in range(pairs):
                    tables_of(t, pair)

                @pl.when(t < devices - 1)
                def _():
                    for pair in range(pairs):
                        table_copy(t, pair).start()

            return carry

        lax.fori_loop(0, devices, one_month, 0)

        totals = []
        for pair in range(pairs):
            total = tab[devices - 1, pair]
            for t in range(devices - 1):
                arrival(t, pair).wait_recv()
                total = total + inbox[t, pair]
            totals.append(total)
        copies = [
            [
                pltpu.make_async_remote_copy(
                    src_ref=mine.at[s],
                    dst_ref=membox.at[de - 1, s],
                    send_sem=msend.at[de - 1, s],
                    recv_sem=mrecv.at[de - 1, s],
                    device_id={"mem": lax.rem(mem + de, members)},
                    device_id_type=pl.DeviceIdType.MESH,
                )
                for de in range(1, members)
            ]
            for s in range(2)
        ]

        def send_part(s):
            for copy in copies[s]:
                copy.start()

        def tail_copy(i, de, dl):
            return pltpu.make_async_remote_copy(
                src_ref=tail,
                dst_ref=tailbox.at[i],
                send_sem=tsend.at[i],
                recv_sem=trecv.at[i],
                device_id={"lat": lax.rem(lat + dl, lats), "mem": lax.rem(mem + de, members)},
                device_id_type=pl.DeviceIdType.MESH,
            )

        def tail_copies(dl):
            return [tail_copy((dl - 1) * members + de, de, dl) for de in range(members)]

        def send_tail(lines):
            for r, line in enumerate(lines):
                tail[r : r + 1, :] = line
            for dl in range(1, lats):

                @pl.when(lat + dl < lats)
                def _():
                    for copy in tail_copies(dl):
                        copy.start()

        month_sums(sz, totals, consts, steps, mine, send_tail, send_part)
        for s in range(2):
            if s == 1:
                for dl in range(1, lats):

                    @pl.when(lat >= dl)
                    def _():
                        for copy in tail_copies(dl):
                            copy.wait_recv()
                        for de in range(members):
                            south[de] = south[de] + tailbox[(dl - 1) * members + de]

            for copy in copies[s]:
                copy.wait_recv()
            for deep in range(2):
                for r in range(REGIONS):
                    at = deep * lanes + r * rows
                    part = []
                    for de in range(members):
                        whole = mine.at[s] if de == 0 else membox.at[de - 1, s]
                        x = whole[at : at + rows, :]
                        if s == 1:
                            x = x + south[de, deep * REGIONS + r : deep * REGIONS + r + 1, :]
                        part.append(x)
                    mean = sum(part[1:], part[0]) / members
                    square = [jnp.square(x - mean) for x in part]
                    at += s * 2 * lanes
                    final[0, at : at + rows, :] = mean
                    final[1, at : at + rows, :] = jnp.sqrt(
                        sum(square[1:], square[0]) / (members - 1)
                    )

        for t in range(devices - 1):
            for pair in range(pairs):
                table_copy(t, pair).wait_send()
        for copy in copies[0] + copies[1]:
            copy.wait_send()
        for dl in range(1, lats):

            @pl.when(lat + dl < lats)
            def _():
                for copy in tail_copies(dl):
                    copy.wait_send()

    arrays = (north_vel, up_vel, dens_class, thickness, basin_id)
    slots = max(1, devices - 1)
    dma = pltpu.SemaphoreType.DMA
    table = (table_rows(sz), 128)
    tails = (2 * REGIONS, wide)
    return pl.pallas_call(
        kernel,
        out_shape=jax.ShapeDtypeStruct((2, tall, wide), F32),
        in_specs=[pl.BlockSpec(memory_space=pl.ANY)] * 5,
        out_specs=pl.BlockSpec(memory_space=pltpu.VMEM),
        scratch_shapes=const_shapes(sz, lons)
        + work_shapes(sz, lons)
        + [
            pltpu.VMEM((months, levels, rows, lons), north_vel.dtype),
            pltpu.VMEM((months, levels, rows, lons), up_vel.dtype),
            pltpu.VMEM((months, levels, rows, lons), dens_class.dtype),
            pltpu.VMEM((levels, rows, lons), thickness.dtype),
            pltpu.VMEM((rows, lons), basin_id.dtype),
            pltpu.VMEM((2, rows, lons), F32),
            pltpu.VMEM((devices, pairs) + table, F32),
            pltpu.VMEM((slots, pairs) + table, F32),
            pltpu.VMEM((2, 2 * lanes, wide), F32),
            pltpu.VMEM((members - 1, 2, 2 * lanes, wide), F32),
            pltpu.VMEM(tails, F32),
            pltpu.VMEM((far,) + tails, F32),
            pltpu.VMEM((members,) + tails, F32),
            dma((devices, pairs, 3)),
            dma((1 + pairs,)),
            dma((slots, pairs)),
            dma((slots, pairs)),
            dma((members - 1, 2)),
            dma((members - 1, 2)),
            dma((far,)),
            dma((far,)),
        ],
        compiler_params=pltpu.CompilerParams(
            collective_id=0, has_side_effects=True, vmem_limit_bytes=44 * 2**20
        ),
    )(*[pltpu.with_memory_space_constraint(x, pltpu.HBM) for x in arrays])


def place(sz, final):
    rows, levels = sz["rows"], sz["levels"]

    def kernel(final, *outs):
        for s in range(2):
            for deep, count in ((1, levels), (0, CLASSES)):
                for i in range(2):
                    for r in range(REGIONS):
                        at = kind_rows(sz, s, deep).start + r * rows
                        o = outs[i + 2 * (1 - deep)]
                        o[0, r, s] = final[i, at : at + rows, :count]

    out = lambda n: jax.ShapeDtypeStruct((1, REGIONS, 2, rows, n), F32)
    outs = pl.pallas_call(
        kernel,
        out_shape=[out(levels), out(levels), out(CLASSES), out(CLASSES)],
        in_specs=[pl.BlockSpec(memory_space=pltpu.VMEM)],
        out_specs=[pl.BlockSpec(memory_space=pltpu.VMEM)] * 4,
        compiler_params=pltpu.CompilerParams(vmem_limit_bytes=8 * 2**20),
    )(final)
    return tuple(jnp.swapaxes(x, 3, 4) for x in outs)


def body(north_vel, up_vel, dens_class, thickness, basin_id):
    levels, rows = north_vel.shape[2:4]
    sz = sizes_of(levels, rows)
    return place(sz, fused(sz, north_vel, up_vel, dens_class, thickness, basin_id))


def solution(mesh):
    in_specs = (
        P("mem", None, None, "lat", "lon"),
        P("mem", None, None, "lat", "lon"),
        P("mem", None, None, "lat", "lon"),
        P(None, "lat", "lon"),
        P("lat", "lon"),
    )
    out_specs = (P("lon", None, None, None, "lat"),) * 4
    return jax.shard_map(body, mesh=mesh, in_specs=in_specs, out_specs=out_specs, check_vma=False)
```

```python
import math

import jax
import jax.numpy as jnp
from jax import lax
from jax.experimental import pallas as pl
from jax.experimental.pallas import tpu as pltpu
from jax.sharding import PartitionSpec as P

CLASSES = 80
BASINS = 3
REGIONS = BASINS + 1
LOW = 32
SUB = 8


north_unit = 0.02
up_unit = 0.01

F32, BF16, F8 = jnp.float32, jnp.bfloat16, jnp.float8_e4m3fn
NT = (((1,), (1,)), ((), ()))
NN = (((1,), (0,)), ((), ()))


def round_up(n, k):
    return -(-n // k) * k


def iota(shape, axis):
    return lax.broadcasted_iota(jnp.int32, shape, axis)


def split(x):
    high = x.astype(BF16)
    return high, (x - high.astype(F32)).astype(BF16)


def exact_dot(ones, x, dims, ones_first=True):
    high, low = split(x)
    if ones_first:
        return lax.dot_general(ones, high, dims, preferred_element_type=F32) + lax.dot_general(
            ones, low, dims, preferred_element_type=F32
        )
    return lax.dot_general(high, ones, dims, preferred_element_type=F32) + lax.dot_general(
        low, ones, dims, preferred_element_type=F32
    )


def sizes_of(levels, rows):
    return dict(
        levels=levels,
        rows=rows,
        pairs=rows // (2 * SUB),
        highs=-(-BASINS * CLASSES // LOW),
        span=-(-CLASSES // LOW),
        near=round_up(-(-levels // 2), 2),
        wide=round_up(max(levels, CLASSES), 128),
        lanes=REGIONS * rows,
    )


def first_high(b):
    return b * CLASSES // LOW


def prepare_weights(sz, consts):
    _, _, upto_class, upto_level, upto_row = consts
    rows = sz["rows"]
    wide = upto_class.shape[2]
    c = iota((SUB, wide), 1)
    for b in range(BASINS):
        for h in range(sz["span"]):
            low = b * CLASSES - (first_high(b) + h) * LOW
            start = max(low, 0)
            stop = jnp.minimum(c + (low + 1), LOW)
            some = stop > start
            beyond = some & (stop > LOW // 2) & (stop < LOW)
            for part in range(LOW // 2):
                both = []
                for half in range(2):
                    target = part if half == 0 else (LOW - part if part else LOW // 2)
                    sign = -1.0 if half == 1 and part else 1.0
                    first = sign if start == target else 0.0
                    x = jnp.where(some, first - jnp.where(stop == target, sign, 0.0), 0.0)
                    if half == 0 and part == 0:
                        if LOW // 2 < start < LOW:
                            x = x + jnp.where(some, 1.0, 0.0)
                        x = x - jnp.where(beyond, 1.0, 0.0)
                    both.append(x)
                at = (h * LOW + 2 * part) * SUB
                upto_class[b, at : at + 2 * SUB, :] = jnp.concatenate(both, 0).astype(BF16)
    shape = upto_level.shape
    upto_level[...] = jnp.where(iota(shape, 0) <= iota(shape, 1), 1.0, 0.0).astype(BF16)
    shape = upto_row.shape
    a, b = iota(shape, 0), iota(shape, 1)
    upto_row[...] = jnp.where((a // rows == b // rows) & (b <= a), 1.0, 0.0).astype(BF16)


def prepare_masks(sz, basin, consts):
    base_ref, mask_ref = consts[:2]
    lons = basin.shape[1]
    base_ref[...] = jnp.where(basin > 0, (basin - 1) * CLASSES, -LOW * 64)
    regions = [basin > 0] + [basin == r for r in range(1, REGIONS)]
    regions = [jnp.where(r, 1.0, 0.0) for r in regions]
    lane = iota((lons, 2 * REGIONS * 2 * SUB), 1)
    none = jnp.zeros(lane.shape, BF16)
    for pair in range(sz["pairs"]):
        cells = slice(pair * 2 * SUB, (pair + 1) * 2 * SUB)
        mask = jnp.concatenate([r[cells] for r in regions] * 2, axis=0).T
        for s in range(2):
            for half in range(2):
                here = (lane // (REGIONS * 2 * SUB) == s) & (lane // SUB % 2 == half)
                here = jnp.where(here, mask, 0.0).astype(BF16)
                for late in range(2):
                    at = (late * 4 + 2 * s + half) * lons
                    mask_ref[pair, at : at + lons, :] = jnp.concatenate(
                        [none, here] if late else [here, none], 1
                    )


def gather_rows(blocks):
    row = iota(blocks[0].shape, 0)
    step = SUB // 2
    while step:
        low = row & step == 0
        joined = []
        for i in range(step):
            x, y = blocks[i], blocks[i + step]
            if step == SUB // 2:
                other = pltpu.roll(jnp.where(low, y, x), step, 0)
            else:
                other = jnp.where(low, pltpu.roll(x, SUB - step, 0), pltpu.roll(y, step, 0))
            joined.append(jnp.where(low, x, y) + other)
        blocks = joined
        step //= 2
    return blocks[0]


def pair_tables(sz, pair, north, up, dens, thick, coef, base_ref, mask_ref, flux, tab):
    highs, levels = sz["highs"], sz["levels"]
    zero = jnp.zeros((2 * SUB, 128), BF16)
    width = LOW * SUB
    own = iota((SUB, 128), 0) == iota((SUB, 128), 1) % SUB
    start = pair * 2 * SUB
    cells = pl.ds(start if isinstance(pair, int) else pl.multiple_of(start, 2 * SUB), 2 * SUB)

    lhs, rhs = ([], []), ([], [])
    kept = None
    for k in range(levels):
        depth_k = thick[k, cells, :].astype(F32)
        nf = north[k, cells, :].astype(F32) * (coef[0, cells, :] * depth_k)
        rf = up[k, cells, :].astype(F32) * (coef[1, cells, :] * jnp.minimum(depth_k, 1.0))
        if k % 2 == 1 or k == levels - 1:
            first = kept if k % 2 == 1 else (nf, rf)
            second = (nf, rf) if k % 2 == 1 else (jnp.zeros_like(nf),) * 2
            for s in range(2):
                for half in range(2):
                    part = slice(half * SUB, (half + 1) * SUB)
                    flux[2 * s + half, pl.ds(k // 2 * 2 * SUB, 2 * SUB), :] = jnp.concatenate(
                        [first[s][part], second[s][part]], 0
                    ).astype(BF16)
        kept = (nf, rf)
        q = base_ref[cells, :] + dens[k, cells, :]
        qf, lo = q.astype(F32), (q & (LOW - 1)).astype(F32)
        for half in range(2):
            part = slice(half * SUB, (half + 1) * SUB)
            join = lambda x, y: jnp.concatenate([x[part], y[part]], 0).astype(BF16)
            at_least = join(qf, qf - LOW)
            ends = join(lo, (LOW - 1) - lo)
            top = jnp.where(join(jnp.full_like(lo, LOW), lo) >= BF16(LOW // 2), BF16(1), zero)
            parts = [top] + [jnp.minimum(ends, BF16(p)) for p in range(1, LOW // 2)]
            rhs[half].append(jnp.concatenate(parts, 0).astype(F8))
            hits = [at_least >= BF16(2 * LOW * p) for p in range(highs // 2)]
            nd, rd = join(nf, nf), join(rf, rf)
            lhs[half].append(
                jnp.concatenate(
                    [jnp.where(h, nd, zero) for h in hits]
                    + [jnp.where(h, rd, zero) for h in hits],
                    0,
                )
            )
    sums = [
        lax.dot_general(
            jnp.concatenate(lhs[half], 1),
            jnp.concatenate(rhs[half], 1),
            NT,
            preferred_element_type=F32,
        )
        for half in range(2)
    ]
    near = sz["near"] * SUB
    seen = lax.dot_general(
        jnp.concatenate([flux[i, late * near : (late + 1) * near, :] for late in range(2) for i in range(4)], 1),
        mask_ref[pair],
        NN,
        preferred_element_type=F32,
    )

    def put(row, blocks):
        tab[row : row + SUB, :] = gather_rows([jnp.where(own, x, 0.0) for x in blocks])

    for half in range(2):
        for s in range(2):
            for c in range(width // 128):
                put(
                    class_row(half, s, c),
                    [
                        sums[half][(s * highs + h) * SUB :, c * 128 : (c + 1) * 128][:SUB]
                        for h in range(highs)
                    ],
                )

    def level(k):
        if k >= levels:
            return jnp.zeros((SUB, 128), F32)
        late, k = divmod(k, sz["near"])
        return seen[k * SUB : (k + 1) * SUB, late * 128 : (late + 1) * 128]

    for k in range(0, levels, SUB):
        put(class_row(2, 0, 0) + k, [level(k + i) for i in range(SUB)])


def class_row(half, s, c):
    return ((half * 2 + s) * (LOW * SUB // 128) + c) * SUB


def table_rows(sz):
    return class_row(2, 0, 0) + round_up(sz["levels"], SUB)


def kind_rows(sz, s, deep):
    at = (2 * s + deep) * sz["lanes"]
    return slice(at, at + sz["lanes"])


def month_sums(sz, total_of, consts, steps, mine, send_tail, send_part):
    _, _, upto_class, upto_level, upto_row = consts
    rows, pairs, highs, span = sz["rows"], sz["pairs"], sz["highs"], sz["span"]
    width, wide = LOW * SUB, sz["wide"]
    row, lane = iota((SUB, 128), 0), iota((SUB, 128), 1)
    own = row == lane % SUB
    deep = []
    for pair in range(pairs):
        total = total_of(pair)
        x = total[class_row(2, 0, 0) :]
        deep.append(jnp.concatenate([x, jnp.zeros((wide - x.shape[0], 128), F32)], 0).T)
        for s in range(2):
            exact = []
            for half in range(2):
                here, back = [], []
                for c in range(width // 128):
                    at = class_row(half, s, c)
                    x = total[at : at + SUB]
                    x = x - jnp.where(row < highs - 1, pltpu.roll(x, SUB - 1, 0), 0.0)
                    here.append(x)
                    back.append(pltpu.roll(x, 2 * SUB, 1))
                for c in range(width // 128):
                    if c == 0:
                        turned = jnp.where(lane < 4 * SUB, 0.0, back[0])
                    else:
                        turned = jnp.where(lane < 2 * SUB, back[c - 1], back[c])
                    x = here[c] - turned
                    high = x.astype(BF16).astype(F32)
                    exact.append((high, x - high))
            for i in range(2):
                for h in range(highs):
                    for c in range(width // 128):
                        both = [exact[half * (width // 128) + c][i] for half in range(2)]
                        both = [
                            jnp.where(own, jnp.broadcast_to(x[h : h + 1], (SUB, 128)), 0.0)
                            for x in both
                        ]
                        at = (i * 2 + s) * rows + pair * 2 * SUB
                        steps[at : at + 2 * SUB, h * width + c * 128 : h * width + (c + 1) * 128] = (
                            jnp.concatenate(both, 0).astype(BF16)
                        )
    found = []
    for b in range(BASINS):
        cols = slice(first_high(b) * width, (first_high(b) + span) * width)
        x = lax.dot_general(steps[:, cols], upto_class[b], NN, preferred_element_type=F32)
        found.append(x[: 2 * rows] + x[2 * rows :])
    found = [sum(found[1:], found[0])] + found
    tables = []
    for s in range(2):
        classes = jnp.concatenate([x[s * rows : (s + 1) * rows] for x in found], 0)
        levels = []
        for r in range(REGIONS):
            for pair in range(pairs):
                at = (s * REGIONS + r) * 2 * SUB
                levels.append(deep[pair][at : at + 2 * SUB])
        tables.append((classes, jnp.concatenate(levels, 0)))
    send_tail(
        [
            jnp.sum(x[r * rows : (r + 1) * rows], axis=0, keepdims=True)
            for x in tables[1]
            for r in range(REGIONS)
        ]
    )
    lanes = sz["lanes"]
    done = [
        (tables[0][0], exact_dot(upto_level[...], tables[0][1], NN, False)),
        tuple(exact_dot(upto_row[...], x, NN) for x in tables[1]),
    ]
    for s in range(2):
        mine[s, :lanes, :], mine[s, lanes:, :] = done[s]
    for s in range(2):
        send_part(s)


def const_shapes(sz, lons):
    lanes, wide = sz["lanes"], sz["wide"]
    return [
        pltpu.VMEM((sz["rows"], lons), jnp.int32),
        pltpu.VMEM((sz["pairs"], 8 * lons, 2 * 2 * REGIONS * 2 * SUB), BF16),
        pltpu.VMEM((BASINS, sz["span"] * LOW * SUB, wide), BF16),
        pltpu.VMEM((wide, wide), BF16),
        pltpu.VMEM((lanes, lanes), BF16),
    ]


def work_shapes(sz, lons):
    return [
        pltpu.VMEM((sz["pairs"], 4, 2 * sz["near"] * SUB, lons), BF16),
        pltpu.VMEM((4 * sz["rows"], sz["highs"] * LOW * SUB), BF16),
    ]


def fused(sz, north_vel, up_vel, dens_class, thickness, basin_id):
    _, months, levels, rows, lons = north_vel.shape
    lanes, wide, pairs = sz["lanes"], sz["wide"], sz["pairs"]
    tall = 4 * lanes
    devices, lats, members = (lax.axis_size(a) for a in ("lon", "lat", "mem"))
    assert months == devices and sz["highs"] == SUB and lons == 128
    far = (lats - 1) * members

    def kernel(north_h, up_h, dens_h, thick_h, basin_h, final, *scratch):
        consts, (flux, steps), rest = scratch[:5], scratch[5:7], scratch[7:]
        (north, up, dens, thick, basin, coef, tab, inbox, mine, membox, tail, tailbox, south) = rest[:13]
        in_sem, fix_sem, send, recv, msend, mrecv, tsend, trecv = rest[13:]
        me, lat, mem = (lax.axis_index(a) for a in ("lon", "lat", "mem"))

        def cells(pair):
            return pl.ds(pl.multiple_of(pair * 2 * SUB, 2 * SUB), 2 * SUB)

        orders = [
            sorted((d for d in range(devices) if d != e), key=lambda d: (d != devices - 1 - e, d))
            for e in range(devices)
        ]

        def month_at(t):
            month = me
            for e, order in enumerate(orders):
                for turn, d in enumerate(order):
                    month = jnp.where((me == e) & (t == turn), d, month)
            return month

        def inputs(t, pair):
            month = month_at(t)
            return [
                pltpu.make_async_copy(
                    h.at[0, month, :, cells(pair), :],
                    v.at[t, :, cells(pair), :],
                    in_sem.at[t, pair, i],
                )
                for i, (h, v) in enumerate(((north_h, north), (up_h, up), (dens_h, dens)))
            ]

        def layers(pair):
            return pltpu.make_async_copy(
                thick_h.at[:, cells(pair), :], thick.at[:, cells(pair), :], fix_sem.at[1 + pair]
            )

        fixed = pltpu.make_async_copy(basin_h, basin, fix_sem.at[0])
        fixed.start()
        layers(0).start()
        for copy in inputs(0, 0):
            copy.start()

        barrier = pltpu.get_barrier_semaphore()
        peers = [{"lon": lax.rem(me + d, devices)} for d in range(1, devices)]
        peers += [
            {"lat": lax.rem(lat + dl, lats), "mem": lax.rem(mem + de, members)}
            for dl in range(lats)
            for de in range(members)
            if dl or de
        ]
        for peer in peers:
            pl.semaphore_signal(
                barrier, inc=1, device_id=peer, device_id_type=pl.DeviceIdType.MESH
            )

        index = lat * rows + iota((rows, lons), 0)
        latitude = (-78.0 + 156.0 * (index.astype(F32) + 0.5) / (rows * lats)) * (math.pi / 180.0)
        zonal = jnp.cos(latitude)
        coef[0] = (north_unit * 0.001) * zonal
        coef[1] = up_unit * zonal
        flux[:, :, levels * SUB :, :] = jnp.zeros_like(flux[:, :, levels * SUB :, :])
        south[...] = jnp.zeros_like(south)
        prepare_weights(sz, consts)
        fixed.wait()
        prepare_masks(sz, basin[...], consts)
        for pair in range(1, pairs):
            for copy in [layers(pair)] + inputs(0, pair):
                copy.start()

        def table_copy(t, pair):
            owner = month_at(t)
            slot = lax.rem(owner - me + devices, devices) - 1
            return pltpu.make_async_remote_copy(
                src_ref=tab.at[t, pair],
                dst_ref=inbox.at[slot, pair],
                send_sem=send.at[t, pair],
                recv_sem=recv.at[slot, pair],
                device_id={"lon": owner},
                device_id_type=pl.DeviceIdType.MESH,
            )

        def arrival(slot, pair):
            return pltpu.make_async_remote_copy(
                src_ref=tab.at[0, pair],
                dst_ref=inbox.at[slot, pair],
                send_sem=send.at[0, pair],
                recv_sem=recv.at[slot, pair],
                device_id={"lon": lax.rem(me + 1, devices)},
                device_id_type=pl.DeviceIdType.MESH,
            )


        def tables_of(t, pair):
            pair_tables(
                sz,
                pair,
                north.at[t],
                up.at[t],
                dens.at[t],
                thick,
                coef,
                consts[0],
                consts[1],
                flux.at[pair],
                tab.at[t, pair],
            )

        def one_month(t, carry):
            @pl.when(t + 1 < devices)
            def _():
                for pair in range(pairs):
                    for copy in inputs(t + 1, pair):
                        copy.start()

            stepwise = (lax.rem(t, 2) == 0) & (t < devices - 1)

            @pl.when(stepwise)
            def _():
                def one_pair(pair, carry):
                    @pl.when(t == 0)
                    def _():
                        layers(pair).wait()

                    for copy in inputs(t, pair):
                        copy.wait()
                    tables_of(t, pair)

                    @pl.when((t == 0) & (pair == pairs - 1))
                    def _():
                        pl.semaphore_wait(barrier, len(peers))
                        for j in range(pairs - 1):
                            table_copy(t, j).start()

                    @pl.when((t > 0) | (pair == pairs - 1))
                    def _():
                        table_copy(t, pair).start()

                    return carry

                lax.fori_loop(0, pairs, one_pair, 0)

            @pl.when(jnp.logical_not(stepwise))
            def _():
                for pair in range(pairs):
                    for copy in inputs(t, pair):
                        copy.wait()
                for pair in range(pairs):
                    tables_of(t, pair)

                @pl.when(t < devices - 1)
                def _():
                    for pair in range(pairs):
                        table_copy(t, pair).start()

            return carry

        lax.fori_loop(0, devices, one_month, 0)

        def total_of(pair):
            total = tab[devices - 1, pair]
            for t in range(devices - 1):
                arrival(t, pair).wait_recv()
                total = total + inbox[t, pair]
            return total

        copies = [
            [
                pltpu.make_async_remote_copy(
                    src_ref=mine.at[s],
                    dst_ref=membox.at[de - 1, s],
                    send_sem=msend.at[de - 1, s],
                    recv_sem=mrecv.at[de - 1, s],
                    device_id={"mem": lax.rem(mem + de, members)},
                    device_id_type=pl.DeviceIdType.MESH,
                )
                for de in range(1, members)
            ]
            for s in range(2)
        ]

        def send_part(s):
            for copy in copies[s]:
                copy.start()

        def tail_copy(i, de, dl):
            return pltpu.make_async_remote_copy(
                src_ref=tail,
                dst_ref=tailbox.at[i],
                send_sem=tsend.at[i],
                recv_sem=trecv.at[i],
                device_id={"lat": lax.rem(lat + dl, lats), "mem": lax.rem(mem + de, members)},
                device_id_type=pl.DeviceIdType.MESH,
            )

        def tail_copies(dl):
            return [tail_copy((dl - 1) * members + de, de, dl) for de in range(members)]

        def send_tail(lines):
            for r, line in enumerate(lines):
                tail[r : r + 1, :] = line
            for dl in range(1, lats):

                @pl.when(lat + dl < lats)
                def _():
                    for copy in tail_copies(dl):
                        copy.start()

        month_sums(sz, total_of, consts, steps, mine, send_tail, send_part)
        for s in range(2):
            if s == 1:
                for dl in range(1, lats):

                    @pl.when(lat >= dl)
                    def _():
                        for copy in tail_copies(dl):
                            copy.wait_recv()
                        for de in range(members):
                            south[de] = south[de] + tailbox[(dl - 1) * members + de]

            for copy in copies[s]:
                copy.wait_recv()
            for deep in range(2):
                for r in range(REGIONS):
                    at = deep * lanes + r * rows
                    part = []
                    for de in range(members):
                        whole = mine.at[s] if de == 0 else membox.at[de - 1, s]
                        x = whole[at : at + rows, :]
                        if s == 1:
                            x = x + south[de, deep * REGIONS + r : deep * REGIONS + r + 1, :]
                        part.append(x)
                    mean = sum(part[1:], part[0]) / members
                    square = [jnp.square(x - mean) for x in part]
                    at += s * 2 * lanes
                    final[0, at : at + rows, :] = mean
                    final[1, at : at + rows, :] = jnp.sqrt(
                        sum(square[1:], square[0]) / (members - 1)
                    )

        for t in range(devices - 1):
            for pair in range(pairs):
                table_copy(t, pair).wait_send()
        for copy in copies[0] + copies[1]:
            copy.wait_send()
        for dl in range(1, lats):

            @pl.when(lat + dl < lats)
            def _():
                for copy in tail_copies(dl):
                    copy.wait_send()

    arrays = (north_vel, up_vel, dens_class, thickness, basin_id)
    slots = max(1, devices - 1)
    dma = pltpu.SemaphoreType.DMA
    table = (table_rows(sz), 128)
    tails = (2 * REGIONS, wide)
    return pl.pallas_call(
        kernel,
        out_shape=jax.ShapeDtypeStruct((2, tall, wide), F32),
        in_specs=[pl.BlockSpec(memory_space=pl.ANY)] * 5,
        out_specs=pl.BlockSpec(memory_space=pltpu.VMEM),
        scratch_shapes=const_shapes(sz, lons)
        + work_shapes(sz, lons)
        + [
            pltpu.VMEM((months, levels, rows, lons), north_vel.dtype),
            pltpu.VMEM((months, levels, rows, lons), up_vel.dtype),
            pltpu.VMEM((months, levels, rows, lons), dens_class.dtype),
            pltpu.VMEM((levels, rows, lons), thickness.dtype),
            pltpu.VMEM((rows, lons), basin_id.dtype),
            pltpu.VMEM((2, rows, lons), F32),
            pltpu.VMEM((devices, pairs) + table, F32),
            pltpu.VMEM((slots, pairs) + table, F32),
            pltpu.VMEM((2, 2 * lanes, wide), F32),
            pltpu.VMEM((members - 1, 2, 2 * lanes, wide), F32),
            pltpu.VMEM(tails, F32),
            pltpu.VMEM((far,) + tails, F32),
            pltpu.VMEM((members,) + tails, F32),
            dma((devices, pairs, 3)),
            dma((1 + pairs,)),
            dma((slots, pairs)),
            dma((slots, pairs)),
            dma((members - 1, 2)),
            dma((members - 1, 2)),
            dma((far,)),
            dma((far,)),
        ],
        compiler_params=pltpu.CompilerParams(
            collective_id=0, has_side_effects=True, vmem_limit_bytes=44 * 2**20
        ),
    )(*[pltpu.with_memory_space_constraint(x, pltpu.HBM) for x in arrays])


def place(sz, final):
    rows, levels = sz["rows"], sz["levels"]

    def kernel(final, *outs):
        for s in range(2):
            for deep, count in ((1, levels), (0, CLASSES)):
                for i in range(2):
                    for r in range(REGIONS):
                        at = kind_rows(sz, s, deep).start + r * rows
                        o = outs[i + 2 * (1 - deep)]
                        o[0, r, s] = final[i, at : at + rows, :count]

    out = lambda n: jax.ShapeDtypeStruct((1, REGIONS, 2, rows, n), F32)
    outs = pl.pallas_call(
        kernel,
        out_shape=[out(levels), out(levels), out(CLASSES), out(CLASSES)],
        in_specs=[pl.BlockSpec(memory_space=pltpu.VMEM)],
        out_specs=[pl.BlockSpec(memory_space=pltpu.VMEM)] * 4,
        compiler_params=pltpu.CompilerParams(vmem_limit_bytes=8 * 2**20),
    )(final)
    return tuple(jnp.swapaxes(x, 3, 4) for x in outs)


def body(north_vel, up_vel, dens_class, thickness, basin_id):
    levels, rows = north_vel.shape[2:4]
    sz = sizes_of(levels, rows)
    return place(sz, fused(sz, north_vel, up_vel, dens_class, thickness, basin_id))


def solution(mesh):
    in_specs = (
        P("mem", None, None, "lat", "lon"),
        P("mem", None, None, "lat", "lon"),
        P("mem", None, None, "lat", "lon"),
        P(None, "lat", "lon"),
        P("lat", "lon"),
    )
    out_specs = (P("lon", None, None, None, "lat"),) * 4
    return jax.shard_map(body, mesh=mesh, in_specs=in_specs, out_specs=out_specs, check_vma=False)
```
